32 devices in a mesh: rows: 4 (over y, x), tp: 8 (over z, core).
Axes of the slice: x: 2, y: 2, z: 4, core: 2. Of those that a mesh axis runs over, the one named last changes fastest.
Arguments:
- train_gate: float32 [3584, 14336], P('rows', 'tp'), may hold values from -0.125 to 0.125
- drift_gate: float32 [3584, 14336], P('rows', 'tp'), may hold values from -6 to 6
- spread_gate: float32 [3584, 14336], P('rows', 'tp'), may hold values from 0.1 to 10
- train_up: float32 [3584, 14336], P('rows', 'tp'), may hold values from -0.125 to 0.125
- drift_up: float32 [3584, 14336], P('rows', 'tp'), may hold values from -6 to 6
- spread_up: float32 [3584, 14336], P('rows', 'tp'), may hold values from 0.1 to 10
- norm_gain: float32 [3584], P('rows'), may hold values from 0.25 to 1.75
Outputs:
- serving_gate: bfloat16 [3584, 14336], P(None, 'tp')
- serving_up: bfloat16 [3584, 14336], P(None, 'tp')
- column_gate: float32 [14336], P('tp')
- column_up: float32 [14336], P('tp')
The draws below stay inside these ranges and needn't reach their ends.
All inputs are finite; a program needn't handle non-finite values. Where the reference program divides by a largest or mean magnitude, that divisor is 1e-20 or more.
Results may differ from the reference program's by a relative error of at most 0.001.
Values may be sent and summed in bfloat16 or wider, within the bound.
A program may use at most 128 MiB of HBM per device.

```python
import math
import jax
import jax.numpy as jnp
from jax import lax

D_MODEL = 3584
D_INNER = 14336


def strengthened(values, rng, source, target, shards_of, factor):
    owner, partner = [(jnp.arange(values.shape[dim]) // (values.shape[dim] // shards_of)).reshape([-1 if axis == dim else 1 for axis in range(values.ndim)]) for dim in (source, target)]
    chosen = jax.random.permutation(rng, shards_of)[partner]
    strong = (owner == chosen) | (owner == (partner + shards_of // 2) % shards_of)
    return jnp.where(strong, factor * values, values)


def steps_of(own_key, shape, shards, low, high):
    def one(axis_at, parts):
        draws = jax.random.uniform(jax.random.fold_in(jax.random.fold_in(own_key, 6), axis_at), (parts,), jnp.float32, low / len(shards), high / len(shards))
        return jnp.repeat(jnp.exp(draws), shape[axis_at] // parts).reshape((-1,) + (1,) * (len(shape) - axis_at - 1))

    gain = one(*shards[0])
    for cut in shards[1:]:
        gain = gain * one(*cut)
    return gain


def bell_draw(own_key, shape, deviation, bound, split=(), dtype=jnp.bfloat16):
    gain = steps_of(own_key, shape, split, -0.22, 0.18) if split else 1.0
    drawn = jax.random.normal(own_key, shape, jnp.float32) * deviation * gain
    return jnp.minimum(jnp.maximum(drawn, -bound), bound).astype(dtype)


def gaussian_with(rng, extent, width, most, shards, heavy, held_as=jnp.bfloat16):
    drawn = width * jax.random.normal(rng, extent, jnp.float32)
    if shards:
        drawn = drawn * steps_of(rng, extent, shards, -0.22, 0.18)
    return jnp.clip(strengthened(drawn, jax.random.fold_in(rng, 3), *heavy), -most, most).astype(held_as)


def setup_inputs(seed: int = 0) -> dict:
    streams_of = jax.random.split(jax.random.key(seed), 8)
    return {
        "train_gate": gaussian_with(streams_of[0], (D_MODEL, D_INNER), D_MODEL ** -0.5, 0.125, ((0, 4), (1, 8)), (0, 1, 8, 2.0), jnp.float32),
        "drift_gate": bell_draw(streams_of[1], (D_MODEL, D_INNER), 1.0, 6.0, ((0, 4), (1, 8)), jnp.float32),
        "spread_gate": jnp.clip(jnp.exp(math.log(10.0) - 4.6051702 * jax.random.uniform(streams_of[2], (D_MODEL, D_INNER), jnp.float32) ** steps_of(streams_of[2], (D_MODEL, D_INNER), ((0, 4), (1, 8)), -0.2, 0.2)), 0.1, 10.0),
        "train_up": gaussian_with(streams_of[3], (D_MODEL, D_INNER), D_MODEL ** -0.5, 0.125, ((0, 4), (1, 8)), (0, 1, 8, 2.0), jnp.float32),
        "drift_up": bell_draw(streams_of[4], (D_MODEL, D_INNER), 1.0, 6.0, ((0, 4), (1, 8)), jnp.float32),
        "spread_up": jnp.clip(jnp.exp(math.log(10.0) - 4.6051702 * jax.random.uniform(streams_of[5], (D_MODEL, D_INNER), jnp.float32) ** steps_of(streams_of[5], (D_MODEL, D_INNER), ((0, 4), (1, 8)), -0.2, 0.2)), 0.1, 10.0),
        "norm_gain": jnp.clip(1.0 + 0.15 * jax.random.normal(streams_of[6], (D_MODEL,), jnp.float32), 0.25, 1.75),
    }


learn_rate = 0.015
decay_rate = 0.1
tiny_value = 1e-08

def reference(train_gate, drift_gate, spread_gate, train_up, drift_up, spread_up, norm_gain):
    whole_gate = train_gate - learn_rate * (drift_gate / (jnp.sqrt(spread_gate) + tiny_value) + decay_rate * train_gate)
    whole_up = train_up - learn_rate * (drift_up / (jnp.sqrt(spread_up) + tiny_value) + decay_rate * train_up)
    whole_gained_gate = whole_gate * norm_gain[:, None]
    whole_gained_up = whole_up * norm_gain[:, None]
    column_gate = lax.optimization_barrier(jnp.max(jnp.abs(whole_gained_gate), axis=0))
    serving_gate = (whole_gained_gate / column_gate).astype(jnp.bfloat16)
    column_up = lax.optimization_barrier(jnp.max(jnp.abs(whole_gained_up), axis=0))
    serving_up = (whole_gained_up / column_up).astype(jnp.bfloat16)
    return (serving_gate, serving_up, column_gate, column_up)
```

```python
import functools
import math

import jax
import jax.numpy as jnp
from jax import lax
from jax.experimental import pallas as pl
from jax.experimental.pallas import tpu as pltpu
from jax.sharding import PartitionSpec as P

learn_rate = 0.015
decay_rate = 0.1
tiny_value = 1e-08
MESH = pl.DeviceIdType.MESH
LANES = 128


def grid_of(rows):
    across = max(d for d in range(1, math.isqrt(rows) + 1) if rows % d == 0)
    return rows // across, across


def block_of(total, options):
    return next(b for b in options if total % b == 0)


def place(rows):
    tall, wide = grid_of(rows)
    me = lax.axis_index("rows")
    turn = lax.rem(lax.axis_index("tp"), 2) if tall == wide else 0
    return me, me // wide, lax.rem(me, wide), turn


def kernel(rows, width, step_rows, late_chunks, *refs):
    ins, gains, outs, columns = refs[:6], refs[6], refs[7:9], refs[9:11]
    late, rest = (refs[11], refs[12:]) if late_chunks else (None, refs[11:])
    stage, whole, peaks, gain = rest[:4]
    in_sem, peak_send, peak_recv, first_send, first_recv, next_send, next_recv = rest[4:]
    tall, wide = grid_of(rows)
    share, total = ins[0].shape
    chunks = total // width
    kept = chunks - late_chunks
    me, my_y, my_x, turn = place(rows)
    lead = (turn, 1 - turn)
    sizes = ((wide, tall), (tall, wide))

    def along_x(k):
        return my_y * wide + lax.rem(my_x + k, wide)

    def along_y(k):
        return lax.rem(my_y + k, tall) * wide + my_x

    def first_peer(m, k):
        return (1 - lead[m]) * along_x(k) + lead[m] * along_y(k)

    def next_peer(m, k):
        return (1 - lead[m]) * along_y(k) + lead[m] * along_x(k)

    def owner_next(m, j, k):
        down = (1 - lead[m]) * k + lead[m] * j
        left = (1 - lead[m]) * j + lead[m] * k
        return lax.rem(my_y + tall - down, tall) * wide + lax.rem(my_x + wide - left, wide)

    def owner_first(m, j):
        return first_peer(m, sizes[m][0] - j) if j else me

    def cols(c):
        return pl.ds(pl.multiple_of(c * width, LANES), width)

    def part(m, owner, c):
        return outs[m].at[pl.ds(pl.multiple_of(owner * share, step_rows), share), cols(c)]

    def load(m, c):
        slot = lax.rem(c, 2)
        return [
            pltpu.make_async_copy(
                ins[3 * m + a].at[:, cols(c)], stage.at[slot, 3 * m + a], in_sem.at[slot, 3 * m + a]
            )
            for a in range(3)
        ]

    def send(src, dst, peer, send_sem, recv_sem):
        return pltpu.make_async_remote_copy(
            src_ref=src, dst_ref=dst, send_sem=send_sem, recv_sem=recv_sem,
            device_id={"rows": peer}, device_id_type=MESH,
        )

    def peak_copy(m, c, k, source, peer):
        ref = peaks.at[m, c, source]
        return send(ref, ref, peer, peak_send.at[m, c, k], peak_recv.at[m, c, k])

    def first_copy(m, c, k, owner, kept_part=True):
        src = part(m, owner, c)
        dst = src if kept_part else late.at[:, cols(c - kept)]
        return send(src, dst, first_peer(m, k), first_send.at[c, m, k], first_recv.at[c, m, k])

    def next_copy(m, j, c, k, owner):
        ref = part(m, owner, c)
        return send(ref, ref, next_peer(m, k), next_send.at[j, c, m, k], next_recv.at[j, c, m, k])

    for copy in load(0, 0):
        copy.start()

    barrier = pltpu.get_barrier_semaphore()
    for k in range(1, rows):
        pl.semaphore_signal(
            barrier, inc=1, device_id={"rows": lax.rem(me + k, rows)}, device_id_type=MESH
        )

    for start in range(0, share, LANES):
        count = min(LANES, share - start)
        line = gains[pl.ds(start, count)].reshape(1, count)
        gain[pl.ds(start, count), :] = jnp.broadcast_to(line, (LANES, count)).T

    for copy in load(1, 0):
        copy.start()

    pl.semaphore_wait(barrier, rows - 1)

    def update(m, c):
        slot = lax.rem(c, 2)
        for copy in load(m, c):
            copy.wait()

        @pl.when(c + 1 < chunks)
        def _():
            for copy in load(m, c + 1):
                copy.start()

        def step(i, most):
            at = pl.ds(pl.multiple_of(i * step_rows, step_rows), step_rows)
            g = gain[at, :]
            found = []
            for t in range(width // LANES):
                lane = pl.ds(t * LANES, LANES)
                train, drift, spread = (stage[slot, 3 * m + a, at, lane] for a in range(3))
                new = train - learn_rate * (
                    drift / (jnp.sqrt(spread) + tiny_value) + decay_rate * train
                )
                new = new * g
                whole[slot, m, at, lane] = new
                tops = jnp.max(jnp.abs(new).reshape(step_rows // 8, 8, LANES), axis=0)
                found.append(jnp.maximum(most[t], tops))
            return tuple(found)

        zero = jnp.zeros((8, LANES), jnp.float32)
        most = lax.fori_loop(0, share // step_rows, step, (zero,) * (width // LANES))
        for t in range(width // LANES):
            peaks[m, c, me, :, pl.ds(t * LANES, LANES)] = jnp.max(most[t], axis=0, keepdims=True)
        for k in range(1, rows):
            peak_copy(m, c, k, me, lax.rem(me + k, rows)).start()

    def finish(m, c):
        slot = lax.rem(c, 2)
        for k in range(1, rows):
            source = lax.rem(me + rows - k, rows)
            peak_copy(m, c, k, source, source).wait_recv()
        scale = peaks[m, c, 0]
        for r in range(1, rows):
            scale = jnp.maximum(scale, peaks[m, c, r])
        columns[m][cols(c)] = scale[0]
        factor = 1.0 / scale

        def step(i, carry):
            at = pl.ds(pl.multiple_of(i * step_rows, step_rows), step_rows)
            to = pl.ds(pl.multiple_of(me * share + i * step_rows, step_rows), step_rows)
            outs[m][to, cols(c)] = (whole[slot, m, at, :] * factor).astype(jnp.bfloat16)
            return carry

        lax.fori_loop(0, share // step_rows, step, 0)
        for k in range(1, sizes[m][0]):
            if m == 0 and late_chunks:

                @pl.when(c < kept)
                def _(k=k):
                    first_copy(m, c, k, me).start()

                @pl.when(c >= kept)
                def _(k=k):
                    first_copy(m, c, k, me, False).start()

            else:
                first_copy(m, c, k, me).start()
        for k in range(1, sizes[m][1]):
            next_copy(m, 0, c, k, me).start()

    def body(c, carry):
        update(0, c)

        @pl.when(c >= 2)
        def _():
            finish(1, c - 2)

        update(1, c)

        @pl.when(c >= 1)
        def _():
            finish(0, c - 1)

        return carry

    lax.fori_loop(0, chunks, body, 0)
    if chunks > 1:
        finish(1, chunks - 2)
    finish(0, chunks - 1)
    finish(1, chunks - 1)

    def forward(m, j, c):
        owner = owner_first(m, j)
        first_copy(m, c, j, owner).wait_recv()
        for k in range(1, sizes[m][1]):
            next_copy(m, j, c, k, owner).start()

    def relay(low, high, late_part):
        def step(c, carry):
            for j in range(1, max(tall, wide)):
                for m in range(2):
                    if j < sizes[m][0]:
                        if m == 0 and late_part:
                            first_copy(m, c, j, me, False).wait_recv()
                        else:
                            forward(m, j, c)
            return carry

        lax.fori_loop(low, high, step, 0)

    relay(0, kept, False)
    if late_chunks:
        relay(kept, chunks, True)

    def drain(c, carry, kept_part=True):
        for m in range(2):
            for k in range(1, rows):
                peak_copy(m, c, k, me, lax.rem(me + k, rows)).wait_send()
            for k in range(1, sizes[m][0]):
                first_copy(m, c, k, me, kept_part or m == 1).wait_send()
            for j in range(sizes[m][0]):
                if j == 0 or m == 1 or kept_part:
                    for k in range(1, sizes[m][1]):
                        next_copy(m, j, c, k, owner_first(m, j)).wait_send()
                        next_copy(m, j, c, k, owner_next(m, j, k)).wait_recv()
        return carry

    lax.fori_loop(0, kept, drain, 0)
    if late_chunks:
        lax.fori_loop(kept, chunks, functools.partial(drain, kept_part=False), 0)


def settle(rows, late_cols, pieces, arrays, late=None):
    ins = arrays + ((late,) if late_cols else ())
    count = len(ins)

    def body(*refs):
        sem = refs[-1]
        copies = []

        def add(src, dst):
            copies.append(pltpu.make_async_copy(src, dst, sem.at[len(copies)]))

        for a in range(len(arrays)):
            src, dst = refs[a], refs[count + a]
            if arrays[a].ndim == 1:
                add(src, dst)
                continue
            tall_share = arrays[a].shape[0] // rows
            tall = tall_share // pieces
            own = arrays[a].shape[1] - late_cols
            if a or not late_cols:
                for p in range(rows * pieces):
                    at = pl.ds(p * tall, tall)
                    add(src.at[at], dst.at[at])
                continue
            me, near, side, far = around(rows)
            for owner, whole in ((me, True), (side, True), (near, False), (far, False)):
                for p in range(pieces):
                    at = pl.ds(pl.multiple_of(owner * tall_share + p * tall, 16), tall)
                    if whole:
                        add(src.at[at], dst.at[at])
                    else:
                        add(src.at[at, pl.ds(0, own)], dst.at[at, pl.ds(0, own)])
            at = pl.ds(pl.multiple_of(near * tall_share, 16), tall_share)
            add(refs[count - 1], dst.at[at, pl.ds(own, late_cols)])
        for copy in copies:
            copy.start()
        for copy in copies:
            copy.wait()

    size = sum(a.size * a.dtype.itemsize for a in arrays)
    return pl.pallas_call(
        body,
        out_shape=tuple(jax.ShapeDtypeStruct(a.shape, a.dtype) for a in arrays),
        in_specs=[pl.BlockSpec(memory_space=pl.ANY)] * count,
        out_specs=(pl.BlockSpec(memory_space=pltpu.HBM),) * len(arrays),
        scratch_shapes=[pltpu.SemaphoreType.DMA((2 * rows * pieces + 3,))],
        compiler_params=pltpu.CompilerParams(vmem_limit_bytes=SMALL),
        cost_estimate=pl.CostEstimate(flops=4 * size, bytes_accessed=2 * size, transcendentals=0),
    )(*ins)


def around(rows):
    me, y, x, turn = place(rows)
    by_x, by_y = y * 2 + (1 - x), (1 - y) * 2 + x
    near = (1 - turn) * by_x + turn * by_y
    side = (1 - turn) * by_y + turn * by_x
    return me, near, side, (1 - y) * 2 + (1 - x)


def complete(rows, served, piece):
    share, late_cols = piece.shape
    own = served.shape[1] - late_cols

    def body(_, src, dst, sem):
        far = around(rows)[3]
        at = pl.ds(pl.multiple_of(far * share, 16), share)
        copy = pltpu.make_async_copy(src, dst.at[at, pl.ds(own, late_cols)], sem)
        copy.start()
        copy.wait()

    return pl.pallas_call(
        body,
        out_shape=jax.ShapeDtypeStruct(served.shape, served.dtype),
        in_specs=[pl.BlockSpec(memory_space=pltpu.HBM), pl.BlockSpec(memory_space=pl.ANY)],
        out_specs=pl.BlockSpec(memory_space=pltpu.HBM),
        scratch_shapes=[pltpu.SemaphoreType.DMA],
        input_output_aliases={0: 0},
        compiler_params=pltpu.CompilerParams(vmem_limit_bytes=SMALL),
    )(served, piece)


def solution(mesh):
    rows, lanes = mesh.shape["rows"], mesh.shape["tp"]

    def per_device(*args):
        arrays, norm_gain = args[:6], args[6]
        share, total = arrays[0].shape
        width = block_of(total, (LANES,))
        step_rows = block_of(share, (32, 16))
        chunks = total // width
        most = max(grid_of(rows))
        late_chunks = LATE if grid_of(rows) == (2, 2) and chunks > LATE else 0
        late_cols = late_chunks * width
        served = pltpu.VMEM((rows * share, total), jnp.bfloat16)
        column = pltpu.VMEM((total,), jnp.float32)
        late = (pltpu.VMEM((share, late_cols), jnp.bfloat16),) if late_chunks else ()
        dma = pltpu.SemaphoreType.DMA
        got = pl.pallas_call(
            functools.partial(kernel, rows, width, step_rows, late_chunks),
            out_shape=(served, served, column, column) + late,
            in_specs=[pl.BlockSpec(memory_space=pltpu.HBM)] * 6
            + [pl.BlockSpec(memory_space=pltpu.VMEM)],
            out_specs=(pl.BlockSpec(memory_space=pltpu.VMEM),) * (4 + len(late)),
            scratch_shapes=[
                pltpu.VMEM((2, 6, share, width), jnp.float32),
                pltpu.VMEM((2, 2, share, width), jnp.float32),
                pltpu.VMEM((2, chunks, rows, 1, width), jnp.float32),
                pltpu.VMEM((share, LANES), jnp.float32),
                dma((2, 6)),
                dma((2, chunks, rows)),
                dma((2, chunks, rows)),
                dma((chunks, 2, most)),
                dma((chunks, 2, most)),
                dma((most, chunks, 2, most)),
                dma((most, chunks, 2, most)),
            ],
            compiler_params=pltpu.CompilerParams(
                collective_id=0, has_side_effects=True, vmem_limit_bytes=VMEM_LIMIT
            ),
        )(*arrays, norm_gain)
        if not late_chunks:
            return settle(rows, 0, 2, got)
        hops = [
            (r * lanes + t, (r ^ (1 if t % 2 else 2)) * lanes + t)
            for r in range(rows)
            for t in range(lanes)
        ]
        piece = lax.ppermute(got[4], ("rows", "tp"), hops)
        done = settle(rows, late_cols, 2, got[:4], got[4])
        return (complete(rows, done[0], piece),) + tuple(done[1:])

    split = P("rows", "tp")
    return jax.shard_map(
        per_device,
        mesh=mesh,
        in_specs=(split,) * 6 + (P("rows"),),
        out_specs=(P(None, "tp"), P(None, "tp"), P("tp"), P("tp")),
        check_vma=False,
    )


LATE = 4
VMEM_LIMIT = 36 * 1024 * 1024
SMALL = 1024 * 1024
```

```python
import functools
import math

import jax
import jax.numpy as jnp
from jax import lax
from jax.experimental import pallas as pl
from jax.experimental.pallas import tpu as pltpu
from jax.sharding import PartitionSpec as P

learn_rate = 0.015
decay_rate = 0.1
tiny_value = 1e-08
MESH = pl.DeviceIdType.MESH
LANES = 128


def grid_of(rows):
    across = max(d for d in range(1, math.isqrt(rows) + 1) if rows % d == 0)
    return rows // across, across


def block_of(total, options):
    return next(b for b in options if total % b == 0)


def place(rows):
    tall, wide = grid_of(rows)
    me = lax.axis_index("rows")
    turn = lax.rem(lax.axis_index("tp"), 2) if tall == wide else 0
    return me, me // wide, lax.rem(me, wide), turn


def kernel(rows, width, step_rows, late_chunks, *refs):
    ins, gains, outs, columns = refs[:6], refs[6], refs[7:9], refs[9:11]
    late, rest = (refs[11:14], refs[14:]) if late_chunks else ((), refs[11:])
    stage, whole, peaks, gain = rest[:4]
    in_sem, peak_send, peak_recv, first_send, first_recv, next_send, next_recv = rest[4:]
    tall, wide = grid_of(rows)
    share, total = ins[0].shape
    chunks = total // width
    kept = chunks - late_chunks
    me, my_y, my_x, turn = place(rows)
    lead = (turn, 1 - turn)
    sizes = ((wide, tall), (tall, wide))

    def along_x(k):
        return my_y * wide + lax.rem(my_x + k, wide)

    def along_y(k):
        return lax.rem(my_y + k, tall) * wide + my_x

    def first_peer(m, k):
        return (1 - lead[m]) * along_x(k) + lead[m] * along_y(k)

    def next_peer(m, k):
        return (1 - lead[m]) * along_y(k) + lead[m] * along_x(k)

    def owner_next(m, j, k):
        down = (1 - lead[m]) * k + lead[m] * j
        left = (1 - lead[m]) * j + lead[m] * k
        return lax.rem(my_y + tall - down, tall) * wide + lax.rem(my_x + wide - left, wide)

    def owner_first(m, j):
        return first_peer(m, sizes[m][0] - j) if j else me

    def cols(c):
        return pl.ds(pl.multiple_of(c * width, LANES), width)

    def part(m, owner, at=None):
        rows_at = pl.ds(pl.multiple_of(owner * share, step_rows), share)
        return outs[m].at[rows_at] if at is None else outs[m].at[rows_at, at]

    def load(m, c):
        slot = lax.rem(c, 2)
        return [
            pltpu.make_async_copy(
                ins[3 * m + a].at[:, cols(c)], stage.at[slot, 3 * m + a], in_sem.at[slot, 3 * m + a]
            )
            for a in range(3)
        ]

    def send(src, dst, peer, send_sem, recv_sem):
        return pltpu.make_async_remote_copy(
            src_ref=src, dst_ref=dst, send_sem=send_sem, recv_sem=recv_sem,
            device_id={"rows": peer}, device_id_type=MESH,
        )

    def peak_copy(m, c, k, source, peer):
        slot = lax.rem(c, SLOTS)
        ref = peaks.at[m, slot, source]
        return send(ref, ref, peer, peak_send.at[m, slot, k - 1], peak_recv.at[m, slot, k - 1])

    def first_copy(m, k, src, dst, group=0):
        return send(src, dst, first_peer(m, k), first_send.at[m, k], first_recv.at[group, m, k])

    def next_copy(m, j, k, ref):
        return send(ref, ref, next_peer(m, k), next_send.at[j, m, k], next_recv.at[j, m, k])

    def last_copy():
        sems = next_send.at[1, 1, 0], next_recv.at[1, 1, 0]
        return send(late[1], late[2], next_peer(1, 1), *sems)

    for copy in load(0, 0):
        copy.start()

    barrier = pltpu.get_barrier_semaphore()
    for k in range(1, rows):
        pl.semaphore_signal(
            barrier, inc=1, device_id={"rows": lax.rem(me + k, rows)}, device_id_type=MESH
        )

    zero = (jnp.zeros((8, LANES), jnp.float32),) * (width // LANES)

    def stepped(m, slot):
        def step(i, most):
            at = pl.ds(pl.multiple_of(i * step_rows, step_rows), step_rows)
            g = gain[at, :]
            found = []
            for t in range(width // LANES):
                lane = pl.ds(t * LANES, LANES)
                train, drift, spread = (stage[slot, 3 * m + a, at, lane] for a in range(3))
                new = train - learn_rate * (
                    drift / (jnp.sqrt(spread) + tiny_value) + decay_rate * train
                )
                new = new * g
                whole[slot, m, at, lane] = new
                tops = jnp.max(jnp.abs(new).reshape(step_rows // 8, 8, LANES), axis=0)
                found.append(jnp.maximum(most[t], tops))
            return tuple(found)

        return lax.fori_loop(0, share // step_rows, step, zero)

    def share_peaks(m, c, most):
        for t in range(width // LANES):
            peaks[m, c % SLOTS, me, :, pl.ds(t * LANES, LANES)] = jnp.max(most[t], axis=0, keepdims=True)

    def send_peaks(m, c):
        for k in range(1, rows):
            peak_copy(m, c, k, me, lax.rem(me + k, rows)).start()

    def wait_peaks(m, c):
        for k in range(1, rows):
            peak_copy(m, c, k, me, lax.rem(me + k, rows)).wait_send()

    for start in range(0, share, LANES):
        count = min(LANES, share - start)
        line = gains[pl.ds(start, count)].reshape(1, count)
        gain[pl.ds(start, count), :] = jnp.broadcast_to(line, (LANES, count)).T

    for copy in load(0, 0):
        copy.wait()
    for copy in load(1, 0):
        copy.start()
    share_peaks(0, 0, stepped(0, 0))
    pl.semaphore_wait(barrier, rows - 1)
    send_peaks(0, 0)
    if chunks > 1:
        for copy in load(0, 1):
            copy.start()

    def update(m, c):
        slot = lax.rem(c, 2)
        for copy in load(m, c):
            copy.wait()

        @pl.when(c + 1 < chunks)
        def _():
            for copy in load(m, c + 1):
                copy.start()

        most = stepped(m, slot)

        @pl.when(c >= SLOTS)
        def _():
            wait_peaks(m, c - SLOTS)

        share_peaks(m, c, most)
        send_peaks(m, c)

    update(1, 0)

    def finish(m, c):
        slot = lax.rem(c, 2)
        for k in range(1, rows):
            source = lax.rem(me + rows - k, rows)
            peak_copy(m, c, k, source, source).wait_recv()
        turn_slot = lax.rem(c, SLOTS)
        scale = peaks[m, turn_slot, 0]
        for r in range(1, rows):
            scale = jnp.maximum(scale, peaks[m, turn_slot, r])
        columns[m][cols(c)] = scale[0]
        factor = 1.0 / scale

        def step(i, carry):
            at = pl.ds(pl.multiple_of(i * step_rows, step_rows), step_rows)
            to = pl.ds(pl.multiple_of(me * share + i * step_rows, step_rows), step_rows)
            outs[m][to, cols(c)] = (whole[slot, m, at, :] * factor).astype(jnp.bfloat16)
            return carry

        lax.fori_loop(0, share // step_rows, step, 0)
        own = part(m, me, cols(c))
        for k in range(1, sizes[m][0]):

            @pl.when(c < kept)
            def _(k=k):
                first_copy(m, k, own, own).start()

            if late_chunks:

                @pl.when(c >= kept)
                def _(k=k):
                    first_copy(m, k, own, late[m].at[:, cols(c - kept)], 1).start()

        for k in range(1, sizes[m][1]):
            next_copy(m, 0, k, own).start()

    def body(c, carry):
        for m in range(2):
            update(m, c)
            finish(m, c - 1)
        return carry

    lax.fori_loop(1, chunks, body, 0)
    for m in range(2):
        finish(m, chunks - 1)

    early = pl.ds(0, kept * width)
    for j in range(1, max(tall, wide)):
        for m in range(2):
            if j < sizes[m][0]:
                block = part(m, owner_first(m, j), early)
                first_copy(m, j, block, block).wait_recv()

    def relay(c, carry):
        for j in range(1, max(tall, wide)):
            for m in range(2):
                if j < sizes[m][0]:
                    for k in range(1, sizes[m][1]):
                        next_copy(m, j, k, part(m, owner_first(m, j), cols(c))).start()
        return carry

    lax.fori_loop(0, kept, relay, 0)
    if late_chunks:
        for m in (1, 0):
            first_copy(m, 1, late[m], late[m], 1).wait_recv()
            if m:
                last_copy().start()

    for m in range(2):
        for c in range(max(0, chunks - SLOTS), chunks):
            wait_peaks(m, c)
        for k in range(1, sizes[m][0]):
            first_copy(m, k, part(m, me), part(m, me)).wait_send()
        for j in range(sizes[m][0]):
            at = early if j else None
            for k in range(1, sizes[m][1]):
                next_copy(m, j, k, part(m, owner_first(m, j), at)).wait_send()
                next_copy(m, j, k, part(m, owner_next(m, j, k), at)).wait_recv()
    if late_chunks:
        last_copy().wait()


def settle(rows, late_cols, pieces, arrays, late=()):
    ins = tuple(arrays) + tuple(late)
    count = len(ins)

    def body(*refs):
        sem = refs[-1]
        copies = []

        def add(src, dst):
            copies.append(pltpu.make_async_copy(src, dst, sem.at[len(copies)]))

        for a in range(len(arrays)):
            src, dst = refs[a], refs[count + a]
            if arrays[a].ndim == 1:
                add(src, dst)
                continue
            share = arrays[a].shape[0] // rows
            tall = share // pieces
            if not late_cols:
                for p in range(rows * pieces):
                    at = pl.ds(p * tall, tall)
                    add(src.at[at], dst.at[at])
                continue
            own = arrays[a].shape[1] - late_cols
            me, near, side, far = around(rows, a)
            for owner, whole in ((me, True), (side, True), (near, False), (far, False)):
                for p in range(pieces):
                    at = pl.ds(pl.multiple_of(owner * share + p * tall, 16), tall)
                    if whole:
                        add(src.at[at], dst.at[at])
                    else:
                        add(src.at[at, pl.ds(0, own)], dst.at[at, pl.ds(0, own)])
            for owner, r in ((near, a), (far, 2))[: a + 1]:
                at = pl.ds(pl.multiple_of(owner * share, 16), share)
                add(refs[len(arrays) + r], dst.at[at, pl.ds(own, late_cols)])
        for copy in copies:
            copy.start()
        for copy in copies:
            copy.wait()

    size = sum(a.size * a.dtype.itemsize for a in arrays)
    return pl.pallas_call(
        body,
        out_shape=tuple(jax.ShapeDtypeStruct(a.shape, a.dtype) for a in arrays),
        in_specs=[pl.BlockSpec(memory_space=pl.ANY)] * count,
        out_specs=(pl.BlockSpec(memory_space=pltpu.HBM),) * len(arrays),
        scratch_shapes=[pltpu.SemaphoreType.DMA((2 * rows * pieces + 5,))],
        compiler_params=pltpu.CompilerParams(vmem_limit_bytes=SMALL),
        cost_estimate=pl.CostEstimate(flops=4 * size, bytes_accessed=2 * size, transcendentals=0),
    )(*ins)


def around(rows, m):
    me, y, x, turn = place(rows)
    turn = 1 - turn if m else turn
    by_x, by_y = y * 2 + (1 - x), (1 - y) * 2 + x
    near = (1 - turn) * by_x + turn * by_y
    side = (1 - turn) * by_y + turn * by_x
    return me, near, side, (1 - y) * 2 + (1 - x)


def complete(rows, served, piece):
    share, late_cols = piece.shape
    own = served.shape[1] - late_cols

    def body(_, src, dst, sem):
        far = around(rows, 0)[3]
        at = pl.ds(pl.multiple_of(far * share, 16), share)
        copy = pltpu.make_async_copy(src, dst.at[at, pl.ds(own, late_cols)], sem)
        copy.start()
        copy.wait()

    return pl.pallas_call(
        body,
        out_shape=jax.ShapeDtypeStruct(served.shape, served.dtype),
        in_specs=[pl.BlockSpec(memory_space=pltpu.HBM), pl.BlockSpec(memory_space=pl.ANY)],
        out_specs=pl.BlockSpec(memory_space=pltpu.HBM),
        scratch_shapes=[pltpu.SemaphoreType.DMA],
        input_output_aliases={0: 0},
        compiler_params=pltpu.CompilerParams(vmem_limit_bytes=SMALL),
    )(served, piece)


def solution(mesh):
    rows, lanes = mesh.shape["rows"], mesh.shape["tp"]

    def per_device(*args):
        arrays, norm_gain = args[:6], args[6]
        share, total = arrays[0].shape
        width = block_of(total, (LANES,))
        step_rows = block_of(share, (32, 16))
        chunks = total // width
        most = max(grid_of(rows))
        late_chunks = LATE if grid_of(rows) == (2, 2) and chunks > LATE else 0
        late_cols = late_chunks * width
        served = pltpu.VMEM((rows * share, total), jnp.bfloat16)
        column = pltpu.VMEM((total,), jnp.float32)
        late = (pltpu.VMEM((share, late_cols), jnp.bfloat16),) * 3 if late_chunks else ()
        dma = pltpu.SemaphoreType.DMA
        got = pl.pallas_call(
            functools.partial(kernel, rows, width, step_rows, late_chunks),
            out_shape=(served, served, column, column) + late,
            in_specs=[pl.BlockSpec(memory_space=pltpu.HBM)] * 6
            + [pl.BlockSpec(memory_space=pltpu.VMEM)],
            out_specs=(pl.BlockSpec(memory_space=pltpu.VMEM),) * (4 + len(late)),
            scratch_shapes=[
                pltpu.VMEM((2, 6, share, width), jnp.float32),
                pltpu.VMEM((2, 2, share, width), jnp.float32),
                pltpu.VMEM((2, SLOTS, rows, 1, width), jnp.float32),
                pltpu.VMEM((share, LANES), jnp.float32),
                dma((2, 6)),
                dma((2, SLOTS, rows - 1)),
                dma((2, SLOTS, rows - 1)),
                dma((2, most)),
                dma((2, 2, most)),
                dma((most, 2, most)),
                dma((most, 2, most)),
            ],
            compiler_params=pltpu.CompilerParams(
                collective_id=0, has_side_effects=True, vmem_limit_bytes=VMEM_LIMIT
            ),
        )(*arrays, norm_gain)
        if not late_chunks:
            return settle(rows, 0, 2, got)
        hops = [
            (r * lanes + t, (r ^ (1 if t % 2 else 2)) * lanes + t)
            for r in range(rows)
            for t in range(lanes)
        ]
        piece = lax.ppermute(got[4], ("rows", "tp"), hops)
        done = settle(rows, late_cols, 2, got[:4], got[4:])
        return (complete(rows, done[0], piece),) + tuple(done[1:])

    split = P("rows", "tp")
    return jax.shard_map(
        per_device,
        mesh=mesh,
        in_specs=(split,) * 6 + (P("rows"),),
        out_specs=(P(None, "tp"), P(None, "tp"), P("tp"), P("tp")),
        check_vma=False,
    )


LATE = 4
SLOTS = 4
VMEM_LIMIT = 30 * 1024 * 1024
SMALL = 1024 * 1024
```

```python
import functools
import math

import jax
import jax.numpy as jnp
from jax import lax
from jax.experimental import pallas as pl
from jax.experimental.pallas import tpu as pltpu
from jax.sharding import PartitionSpec as P

learn_rate = 0.015
decay_rate = 0.1
tiny_value = 1e-08
MESH = pl.DeviceIdType.MESH
LANES = 128


def grid_of(rows):
    across = max(d for d in range(1, math.isqrt(rows) + 1) if rows % d == 0)
    return rows // across, across


def block_of(total, options):
    return next(b for b in options if total % b == 0)


def place(rows):
    tall, wide = grid_of(rows)
    me = lax.axis_index("rows")
    turn = lax.rem(lax.axis_index("tp"), 2) if tall == wide else 0
    return me, me // wide, lax.rem(me, wide), turn


def kernel(rows, width, step_rows, held, gone, *refs):
    ins, gains, outs, columns = refs[:6], refs[6], refs[7:9], refs[9:11]
    sides, rest = (refs[11:17], refs[17:]) if gone else ((), refs[11:])
    near, far, late = sides[:2], sides[2:4], sides[4:]
    stage, whole, peaks, gain = rest[:4]
    in_sem, peak_send, peak_recv, first_send, first_recv, next_send, next_recv = rest[4:11]
    if gone:
        held_send, held_recv, go = rest[11:]
    tall, wide = grid_of(rows)
    share, total = ins[0].shape
    chunks = total // width
    kept = chunks - held - gone
    me, my_y, my_x, turn = place(rows)
    tp = lax.axis_index("tp")
    lead = (turn, 1 - turn)
    sizes = ((wide, tall), (tall, wide))

    def along_x(k):
        return my_y * wide + lax.rem(my_x + k, wide)

    def along_y(k):
        return lax.rem(my_y + k, tall) * wide + my_x

    def first_peer(m, k):
        return (1 - lead[m]) * along_x(k) + lead[m] * along_y(k)

    def next_peer(m, k):
        return (1 - lead[m]) * along_y(k) + lead[m] * along_x(k)

    def owner_next(m, j, k):
        down = (1 - lead[m]) * k + lead[m] * j
        left = (1 - lead[m]) * j + lead[m] * k
        return lax.rem(my_y + tall - down, tall) * wide + lax.rem(my_x + wide - left, wide)

    def owner_first(m, j):
        return first_peer(m, sizes[m][0] - j) if j else me

    def cols(c):
        return pl.ds(pl.multiple_of(c * width, LANES), width)

    def part(m, owner, at=None):
        rows_at = pl.ds(pl.multiple_of(owner * share, step_rows), share)
        return outs[m].at[rows_at] if at is None else outs[m].at[rows_at, at]

    def load(m, c, pieces=1):
        slot = lax.rem(c, 2)
        tall_piece = share // pieces
        return [
            pltpu.make_async_copy(
                ins[3 * m + a].at[pl.ds(p * tall_piece, tall_piece), cols(c)],
                stage.at[slot, 3 * m + a, pl.ds(p * tall_piece, tall_piece)],
                in_sem.at[slot, m],
            )
            for p in range(pieces)
            for a in range(3)
        ]

    def wait_load(m, c):
        slot = lax.rem(c, 2)
        block = stage.at[slot, pl.ds(3 * m, 3)]
        pltpu.make_async_copy(block, block, in_sem.at[slot, m]).wait()

    def send(src, dst, peer, send_sem, recv_sem):
        return pltpu.make_async_remote_copy(
            src_ref=src, dst_ref=dst, send_sem=send_sem, recv_sem=recv_sem,
            device_id={"rows": peer}, device_id_type=MESH,
        )

    def peak_copy(m, c, k):
        slot = lax.rem(c, SLOTS)
        ref = peaks.at[m, slot, me]
        return send(ref, ref, lax.rem(me + k, rows), peak_send.at[m, slot], peak_recv.at[m, slot])

    def all_peaks(m, c):
        slot = lax.rem(c, SLOTS)
        ref = peaks.at[m, slot, pl.ds(0, rows - 1)]
        return send(ref, ref, lax.rem(me + 1, rows), peak_send.at[m, slot], peak_recv.at[m, slot])

    def first_copy(m, k, src, dst, group=0):
        sems = first_send.at[m, k - 1], first_recv.at[group, m, k - 1]
        return send(src, dst, first_peer(m, k), *sems)

    def next_copy(m, j, k, ref):
        return send(ref, ref, next_peer(m, k), next_send.at[j, m, k - 1], next_recv.at[j, m, k - 1])

    def held_copy(m, half):
        at = pl.ds(half * (share // 2), share // 2)
        sems = held_send.at[m, half], held_recv.at[m, half]
        return send(near[m].at[at], far[m].at[at], next_peer(m, 1), *sems)

    for copy in load(0, 0, block_of(share, (7, 1)) if share % 112 == 0 else 1):
        copy.start()

    barrier = pltpu.get_barrier_semaphore()
    for k in range(1, rows):
        pl.semaphore_signal(
            barrier, inc=1, device_id={"rows": lax.rem(me + k, rows)}, device_id_type=MESH
        )

    if gone:
        sibling = {"tp": tp + 1 - 2 * turn}
        pl.semaphore_signal(barrier, inc=1, device_id=sibling, device_id_type=MESH)

    zero = (jnp.zeros((8, LANES), jnp.float32),) * (width // LANES)

    def stepped(m, slot):
        def step(i, most):
            at = pl.ds(pl.multiple_of(i * step_rows, step_rows), step_rows)
            g = gain[at, :]
            found = []
            for t in range(width // LANES):
                lane = pl.ds(t * LANES, LANES)
                train, drift, spread = (stage[slot, 3 * m + a, at, lane] for a in range(3))
                new = train - learn_rate * (
                    drift / (jnp.sqrt(spread) + tiny_value) + decay_rate * train
                )
                new = new * g
                whole[slot, m, at, lane] = new
                tops = jnp.max(jnp.abs(new).reshape(step_rows // 8, 8, LANES), axis=0)
                found.append(jnp.maximum(most[t], tops))
            return tuple(found)

        return lax.fori_loop(0, share // step_rows, step, zero)

    def share_peaks(m, c, most):
        for t in range(width // LANES):
            peaks[m, c % SLOTS, me, :, pl.ds(t * LANES, LANES)] = jnp.max(most[t], axis=0, keepdims=True)

    def send_peaks(m, c):
        for k in range(1, rows):
            peak_copy(m, c, k).start()

    for start in range(0, share, LANES):
        count = min(LANES, share - start)
        line = gains[pl.ds(start, count)].reshape(1, count)
        gain[pl.ds(start, count), :] = jnp.broadcast_to(line, (LANES, count)).T

    wait_load(0, 0)
    for copy in load(1, 0):
        copy.start()
    share_peaks(0, 0, stepped(0, 0))
    pl.semaphore_wait(barrier, rows if gone else rows - 1)
    send_peaks(0, 0)
    if chunks > 1:
        for copy in load(0, 1):
            copy.start()

    def update(m, c):
        slot = lax.rem(c, 2)
        wait_load(m, c)

        @pl.when(c + 1 < chunks)
        def _():
            for copy in load(m, c + 1):
                copy.start()

        most = stepped(m, slot)

        @pl.when(c >= SLOTS)
        def _():
            all_peaks(m, c - SLOTS).wait_send()

        share_peaks(m, c, most)
        send_peaks(m, c)

    update(1, 0)

    def finish(m, c):
        slot = lax.rem(c, 2)
        all_peaks(m, c).wait_recv()
        turn_slot = lax.rem(c, SLOTS)
        scale = peaks[m, turn_slot, 0]
        for r in range(1, rows):
            scale = jnp.maximum(scale, peaks[m, turn_slot, r])
        columns[m][cols(c)] = scale[0]
        factor = 1.0 / scale

        def step(i, carry):
            at = pl.ds(pl.multiple_of(i * step_rows, step_rows), step_rows)
            to = pl.ds(pl.multiple_of(me * share + i * step_rows, step_rows), step_rows)
            outs[m][to, cols(c)] = (whole[slot, m, at, :] * factor).astype(jnp.bfloat16)
            return carry

        lax.fori_loop(0, share // step_rows, step, 0)
        own = part(m, me, cols(c))
        for k in range(1, sizes[m][0]):

            @pl.when(c < kept)
            def _(k=k):
                first_copy(m, k, own, own).start()

            if gone:

                @pl.when((c >= kept) & (c < kept + held))
                def _(k=k):
                    first_copy(m, k, own, near[m].at[:, cols(c - kept)], 1).start()

                @pl.when(c >= kept + held)
                def _(k=k):
                    first_copy(m, k, own, late[m].at[:, cols(c - kept - held)], 2).start()

        for k in range(1, sizes[m][1]):
            next_copy(m, 0, k, own).start()

    def body(c, carry):
        for m in range(2):
            update(m, c)
            finish(m, c - 1)
        return carry

    lax.fori_loop(1, chunks, body, 0)
    for m in range(2):
        finish(m, chunks - 1)

    early = pl.ds(0, kept * width)
    for j in range(1, max(tall, wide)):
        for m in range(2):
            if j < sizes[m][0]:
                block = part(m, owner_first(m, j), early)
                first_copy(m, j, block, block).wait_recv()

    def relay(c, carry):
        for j in range(1, max(tall, wide)):
            for m in range(2):
                if j < sizes[m][0]:
                    for k in range(1, sizes[m][1]):
                        next_copy(m, j, k, part(m, owner_first(m, j), cols(c))).start()
        return carry

    lax.fori_loop(0, kept, relay, 0)
    if gone:
        for m in range(2):
            first_copy(m, 1, near[m], near[m], 1).wait_recv()

        @pl.when(turn == 1)
        def _():
            pl.semaphore_wait(go, 1)

        for half in range(2):
            for m in range(2):
                held_copy(m, half).start()
        for m in range(2):
            held_copy(m, 0).wait_send()

        @pl.when(turn == 0)
        def _():
            pl.semaphore_signal(go, inc=1, device_id=sibling, device_id_type=MESH)

        for m in range(2):
            first_copy(m, 1, late[m], late[m], 2).wait_recv()

    for m in range(2):
        for c in range(max(0, chunks - SLOTS), chunks):
            all_peaks(m, c).wait_send()
        for k in range(1, sizes[m][0]):
            first_copy(m, k, part(m, me), part(m, me)).wait_send()
        for j in range(sizes[m][0]):
            at = early if j else None
            for k in range(1, sizes[m][1]):
                next_copy(m, j, k, part(m, owner_first(m, j), at)).wait_send()
                next_copy(m, j, k, part(m, owner_next(m, j, k), at)).wait_recv()
    if gone:
        for m in range(2):
            held_copy(m, 1).wait_send()
            for half in range(2):
                held_copy(m, half).wait_recv()


def settle(rows, held_cols, late_cols, pieces, arrays, sides=()):
    ins = tuple(arrays) + tuple(sides)
    count = len(ins)

    def body(*refs):
        sem = refs[-1]
        near, far, late = refs[4:6], refs[6:8], refs[8:10]
        copies = []

        def add(src, dst):
            copies.append(pltpu.make_async_copy(src, dst, sem.at[len(copies)]))

        for a in range(len(arrays)):
            src, dst = refs[a], refs[count + a]
            if arrays[a].ndim == 1:
                add(src, dst)
                continue
            share = arrays[a].shape[0] // rows
            tall = share // pieces
            if not late_cols:
                for p in range(rows * pieces):
                    at = pl.ds(p * tall, tall)
                    add(src.at[at], dst.at[at])
                continue
            own = arrays[a].shape[1] - late_cols - held_cols
            me, first, second, last = around(rows, a)
            for owner, whole in ((me, True), (second, True), (first, False), (last, False)):
                for p in range(pieces):
                    at = pl.ds(pl.multiple_of(owner * share + p * tall, 16), tall)
                    if whole:
                        add(src.at[at], dst.at[at])
                    else:
                        add(src.at[at, pl.ds(0, own)], dst.at[at, pl.ds(0, own)])
            first_at = pl.ds(pl.multiple_of(first * share, 16), share)
            last_at = pl.ds(pl.multiple_of(last * share, 16), share)
            add(near[a], dst.at[first_at, pl.ds(own, held_cols)])
            add(late[a], dst.at[first_at, pl.ds(own + held_cols, late_cols)])
            add(far[a], dst.at[last_at, pl.ds(own, held_cols)])
        for copy in copies:
            copy.start()
        for copy in copies:
            copy.wait()

    size = sum(a.size * a.dtype.itemsize for a in arrays)
    return pl.pallas_call(
        body,
        out_shape=tuple(jax.ShapeDtypeStruct(a.shape, a.dtype) for a in arrays),
        in_specs=[pl.BlockSpec(memory_space=pl.ANY)] * count,
        out_specs=(pl.BlockSpec(memory_space=pltpu.HBM),) * len(arrays),
        scratch_shapes=[pltpu.SemaphoreType.DMA((2 * rows * pieces + 8,))],
        compiler_params=pltpu.CompilerParams(vmem_limit_bytes=SMALL),
        cost_estimate=pl.CostEstimate(flops=4 * size, bytes_accessed=2 * size, transcendentals=0),
    )(*ins)


def around(rows, m):
    me, y, x, turn = place(rows)
    turn = 1 - turn if m else turn
    by_x, by_y = y * 2 + (1 - x), (1 - y) * 2 + x
    near = (1 - turn) * by_x + turn * by_y
    side = (1 - turn) * by_y + turn * by_x
    return me, near, side, (1 - y) * 2 + (1 - x)


def complete(rows, served, late):
    share, late_cols = late[0].shape
    own = served[0].shape[1] - late_cols

    def body(*refs):
        sem = refs[-1]
        copies = []
        for m in range(2):
            at = pl.ds(pl.multiple_of(around(rows, m)[3] * share, 16), share)
            dst = refs[4 + m].at[at, pl.ds(own, late_cols)]
            copies.append(pltpu.make_async_copy(refs[2 + m], dst, sem.at[m]))
        for copy in copies:
            copy.start()
        for copy in copies:
            copy.wait()

    return pl.pallas_call(
        body,
        out_shape=tuple(jax.ShapeDtypeStruct(a.shape, a.dtype) for a in served),
        in_specs=[pl.BlockSpec(memory_space=pltpu.HBM)] * 2
        + [pl.BlockSpec(memory_space=pl.ANY)] * 2,
        out_specs=(pl.BlockSpec(memory_space=pltpu.HBM),) * 2,
        scratch_shapes=[pltpu.SemaphoreType.DMA((2,))],
        input_output_aliases={0: 0, 1: 1},
        compiler_params=pltpu.CompilerParams(vmem_limit_bytes=SMALL),
    )(*served, *late)


def solution(mesh):
    rows, lanes = mesh.shape["rows"], mesh.shape["tp"]

    def per_device(*args):
        arrays, norm_gain = args[:6], args[6]
        share, total = arrays[0].shape
        width = block_of(total, (LANES,))
        step_rows = block_of(share, (32, 16))
        chunks = total // width
        most = max(grid_of(rows))
        split = grid_of(rows) == (2, 2) and lanes % 2 == 0 and chunks > HELD + LATE
        held, gone = (HELD, LATE) if split else (0, 0)
        served = pltpu.VMEM((rows * share, total), jnp.bfloat16)
        column = pltpu.VMEM((total,), jnp.float32)
        sides = ()
        dma = pltpu.SemaphoreType.DMA
        more = []
        if split:
            held_side = pltpu.VMEM((share, held * width), jnp.bfloat16)
            sides = (held_side,) * 4 + (pltpu.VMEM((share, gone * width), jnp.bfloat16),) * 2
            more = [dma((2, 2)), dma((2, 2)), pltpu.SemaphoreType.REGULAR]
        got = pl.pallas_call(
            functools.partial(kernel, rows, width, step_rows, held, gone),
            out_shape=(served, served, column, column) + sides,
            in_specs=[pl.BlockSpec(memory_space=pltpu.HBM)] * 6
            + [pl.BlockSpec(memory_space=pltpu.VMEM)],
            out_specs=(pl.BlockSpec(memory_space=pltpu.VMEM),) * (4 + len(sides)),
            scratch_shapes=[
                pltpu.VMEM((2, 6, share, width), jnp.float32),
                pltpu.VMEM((2, 2, share, width), jnp.float32),
                pltpu.VMEM((2, SLOTS, rows, 1, width), jnp.float32),
                pltpu.VMEM((share, LANES), jnp.float32),
                dma((2, 2)),
                dma((2, SLOTS)),
                dma((2, SLOTS)),
                dma((2, most - 1)),
                dma((3 if split else 1, 2, most - 1)),
                dma((most, 2, most - 1)),
                dma((most, 2, most - 1)),
            ]
            + more,
            compiler_params=pltpu.CompilerParams(
                collective_id=0, has_side_effects=True, vmem_limit_bytes=VMEM_LIMIT
            ),
        )(*arrays, norm_gain)
        if not split:
            return settle(rows, 0, 0, 2, got)

        def hop(m, late):
            hops = [
                (r * lanes + t, (r ^ (1 if (t + m) % 2 else 2)) * lanes + t)
                for r in range(rows)
                for t in range(lanes)
            ]
            return lax.ppermute(late, ("rows", "tp"), hops)

        late = [hop(m, got[8 + m]) for m in range(2)]
        done = settle(rows, held * width, gone * width, 2, got[:4], got[4:])
        return tuple(complete(rows, done[:2], late)) + tuple(done[2:])

    split = P("rows", "tp")
    return jax.shard_map(
        per_device,
        mesh=mesh,
        in_specs=(split,) * 6 + (P("rows"),),
        out_specs=(P(None, "tp"), P(None, "tp"), P("tp"), P("tp")),
        check_vma=False,
    )


HELD = 2
LATE = 3
SLOTS = 4
VMEM_LIMIT = 30 * 1024 * 1024
SMALL = 1024 * 1024
```

```python
import functools
import math

import jax
import jax.numpy as jnp
from jax import lax
from jax.experimental import pallas as pl
from jax.experimental.pallas import tpu as pltpu
from jax.sharding import PartitionSpec as P

learn_rate = 0.015
decay_rate = 0.1
tiny_value = 1e-08
MESH = pl.DeviceIdType.MESH
LANES = 128


def grid_of(rows):
    across = max(d for d in range(1, math.isqrt(rows) + 1) if rows % d == 0)
    return rows // across, across


def block_of(total, options):
    return next(b for b in options if total % b == 0)


def place(rows):
    tall, wide = grid_of(rows)
    me = lax.axis_index("rows")
    turn = lax.rem(lax.axis_index("tp"), 2) if tall == wide else 0
    return me, me // wide, lax.rem(me, wide), turn


def kernel(rows, width, step_rows, held, gone, *refs):
    ins, gains, outs, columns = refs[:6], refs[6], refs[7:9], refs[9:11]
    sides, rest = (refs[11:17], refs[17:]) if gone else ((), refs[11:])
    near, far, late = sides[:2], sides[2:4], sides[4:]
    stage, whole, peaks, gain = rest[:4]
    in_sem, piece_sem, peak_send, peak_recv = rest[4:8]
    first_send, first_recv, next_send, next_recv = rest[8:12]
    if gone:
        held_send, held_recv, go, early, early_send, early_recv, rest_send, rest_recv = rest[12:]
    tall, wide = grid_of(rows)
    share, total = ins[0].shape
    chunks = total // width
    kept = chunks - held - gone
    me, my_y, my_x, turn = place(rows)
    tp = lax.axis_index("tp")
    lead = (turn, 1 - turn)
    sizes = ((wide, tall), (tall, wide))

    def along_x(k):
        return my_y * wide + lax.rem(my_x + k, wide)

    def along_y(k):
        return lax.rem(my_y + k, tall) * wide + my_x

    def first_peer(m, k):
        return (1 - lead[m]) * along_x(k) + lead[m] * along_y(k)

    def next_peer(m, k):
        return (1 - lead[m]) * along_y(k) + lead[m] * along_x(k)

    def owner_next(m, j, k):
        down = (1 - lead[m]) * k + lead[m] * j
        left = (1 - lead[m]) * j + lead[m] * k
        return lax.rem(my_y + tall - down, tall) * wide + lax.rem(my_x + wide - left, wide)

    def owner_first(m, j):
        return first_peer(m, sizes[m][0] - j) if j else me

    def cols(c):
        return pl.ds(pl.multiple_of(c * width, LANES), width)

    def part(m, owner, at):
        return outs[m].at[pl.ds(pl.multiple_of(owner * share, step_rows), share), at]

    def load(m, c):
        slot = lax.rem(c, 2)
        return [
            pltpu.make_async_copy(
                ins[3 * m + a].at[:, cols(c)], stage.at[slot, 3 * m + a], in_sem.at[slot, m]
            )
            for a in range(3)
        ]

    def wait_load(m, c):
        slot = lax.rem(c, 2)
        block = stage.at[slot, pl.ds(3 * m, 3)]
        pltpu.make_async_copy(block, block, in_sem.at[slot, m]).wait()

    def send(src, dst, peer, send_sem, recv_sem):
        return pltpu.make_async_remote_copy(
            src_ref=src, dst_ref=dst, send_sem=send_sem, recv_sem=recv_sem,
            device_id={"rows": peer}, device_id_type=MESH,
        )

    def peak_copy(m, c, k):
        slot = lax.rem(c, SLOTS)
        ref = peaks.at[m, slot, me]
        return send(ref, ref, lax.rem(me + k, rows), peak_send.at[m, slot], peak_recv.at[m, slot])

    def all_peaks(m, c):
        slot = lax.rem(c, SLOTS)
        ref = peaks.at[m, slot, pl.ds(0, rows - 1)]
        return send(ref, ref, lax.rem(me + 1, rows), peak_send.at[m, slot], peak_recv.at[m, slot])

    def first_copy(m, k, src, dst, group=0):
        sems = first_send.at[m, k - 1], first_recv.at[group, m, k - 1]
        return send(src, dst, first_peer(m, k), *sems)

    def next_copy(m, j, k, ref):
        return send(ref, ref, next_peer(m, k), next_send.at[j, m, k - 1], next_recv.at[j, m, k - 1])

    def held_copy(m, half):
        at = pl.ds(half * (share // 2), share // 2)
        sems = held_send.at[m, half], held_recv.at[m, half]
        return send(near[m].at[at], far[m].at[at], next_peer(m, 1), *sems)

    def early_copy(side):
        src, dst = whole.at[0, 0, pl.ds(0, EARLY)], early.at[side]
        peer = (first_peer, next_peer)[side](0, 1)
        return send(src, dst, peer, early_send.at[side], early_recv.at[side])

    def rest_copy(side, owner):
        at = pl.ds(pl.multiple_of(owner * share + EARLY, step_rows), share - EARLY)
        ref = outs[0].at[at, cols(0)]
        peer = (first_peer, next_peer)[side](0, 1)
        return send(ref, ref, peer, rest_send.at[side], rest_recv.at[side])

    pieces = piece_sem.shape[0]
    tall_piece = share // pieces
    for p in range(pieces):
        at = pl.ds(p * tall_piece, tall_piece)
        for a in range(3):
            pltpu.make_async_copy(
                ins[a].at[at, cols(0)], stage.at[0, a, at], piece_sem.at[p]
            ).start()

    barrier = pltpu.get_barrier_semaphore()
    for k in range(1, rows):
        pl.semaphore_signal(
            barrier, inc=1, device_id={"rows": lax.rem(me + k, rows)}, device_id_type=MESH
        )

    if gone:
        sibling = {"tp": tp + 1 - 2 * turn}
        pl.semaphore_signal(barrier, inc=1, device_id=sibling, device_id_type=MESH)

    zero = (jnp.zeros((8, LANES), jnp.float32),) * (width // LANES)

    def stepped(m, slot, low, high, most):
        def step(i, most):
            at = pl.ds(pl.multiple_of(i * step_rows, step_rows), step_rows)
            g = gain[at, :]
            found = []
            for t in range(width // LANES):
                lane = pl.ds(t * LANES, LANES)
                train, drift, spread = (stage[slot, 3 * m + a, at, lane] for a in range(3))
                new = train - learn_rate * (
                    drift / (jnp.sqrt(spread) + tiny_value) + decay_rate * train
                )
                new = new * g
                whole[slot, m, at, lane] = new
                tops = jnp.max(jnp.abs(new).reshape(step_rows // 8, 8, LANES), axis=0)
                found.append(jnp.maximum(most[t], tops))
            return tuple(found)

        return lax.fori_loop(low // step_rows, high // step_rows, step, most)

    def share_peaks(m, c, most):
        for t in range(width // LANES):
            peaks[m, c % SLOTS, me, :, pl.ds(t * LANES, LANES)] = jnp.max(most[t], axis=0, keepdims=True)

    def send_peaks(m, c):
        for k in range(1, rows):
            peak_copy(m, c, k).start()

    for start in range(0, share, LANES):
        count = min(LANES, share - start)
        line = gains[pl.ds(start, count)].reshape(1, count)
        gain[pl.ds(start, count), :] = jnp.broadcast_to(line, (LANES, count)).T

    most = zero
    for p in range(pieces):
        block = stage.at[0, pl.ds(0, 3), pl.ds(p * tall_piece, tall_piece)]
        pltpu.make_async_copy(block, block, piece_sem.at[p]).wait()
        if p == pieces // 2:
            for copy in load(1, 0):
                copy.start()
        most = stepped(0, 0, p * tall_piece, (p + 1) * tall_piece, most)
    share_peaks(0, 0, most)
    pl.semaphore_wait(barrier, rows if gone else rows - 1)
    send_peaks(0, 0)
    if gone:
        for side in range(2):
            early_copy(side).start()
    if chunks > 1:
        for copy in load(0, 1):
            copy.start()

    def update(m, c):
        slot = lax.rem(c, 2)
        wait_load(m, c)

        @pl.when(c + 1 < chunks)
        def _():
            for copy in load(m, c + 1):
                copy.start()

        most = stepped(m, slot, 0, share, zero)

        @pl.when(c >= SLOTS)
        def _():
            all_peaks(m, c - SLOTS).wait_send()

        share_peaks(m, c, most)
        send_peaks(m, c)

    update(1, 0)

    def finish(m, c, split=False):
        slot = lax.rem(c, 2)
        all_peaks(m, c).wait_recv()
        turn_slot = lax.rem(c, SLOTS)
        scale = peaks[m, turn_slot, 0]
        for r in range(1, rows):
            scale = jnp.maximum(scale, peaks[m, turn_slot, r])
        columns[m][cols(c)] = scale[0]
        factor = 1.0 / scale

        def step(i, carry):
            at = pl.ds(pl.multiple_of(i * step_rows, step_rows), step_rows)
            to = pl.ds(pl.multiple_of(me * share + i * step_rows, step_rows), step_rows)
            outs[m][to, cols(c)] = (whole[slot, m, at, :] * factor).astype(jnp.bfloat16)
            return carry

        lax.fori_loop(0, share // step_rows, step, 0)
        if split:
            for side in range(2):
                rest_copy(side, me).start()
            return
        own = part(m, me, cols(c))
        for k in range(1, sizes[m][0]):

            @pl.when(c < kept)
            def _(k=k):
                first_copy(m, k, own, own).start()

            if gone:

                @pl.when((c >= kept) & (c < kept + held))
                def _(k=k):
                    first_copy(m, k, own, near[m].at[:, cols(c - kept)], 1).start()

                @pl.when(c >= kept + held)
                def _(k=k):
                    first_copy(m, k, own, late[m].at[:, cols(c - kept - held)], 2).start()

        for k in range(1, sizes[m][1]):
            next_copy(m, 0, k, own).start()

    def body(c, carry):
        for m in range(2):
            update(m, c)
            finish(m, c - 1)
        return carry

    if gone:
        update(0, 1)
        finish(0, 0, True)
        update(1, 1)
        finish(1, 0)
        for side in range(2):
            early_copy(side).wait_send()
    lax.fori_loop(2 if gone else 1, chunks, body, 0)
    for m in range(2):
        finish(m, chunks - 1)

    apart = width if gone else 0

    def span(m, j):
        low = apart if j == 0 and m == 0 else 0
        high = total if j == 0 else kept * width
        return pl.ds(low, high - low)

    if gone:
        factor = 1.0 / columns[0][cols(0)].reshape(1, width)
        for side in range(2):
            owner = (first_peer, next_peer)[side](0, 1)
            early_copy(side).wait_recv()

            def scale_step(i, carry, side=side, owner=owner):
                at = pl.ds(pl.multiple_of(i * step_rows, step_rows), step_rows)
                to = pl.ds(pl.multiple_of(owner * share + i * step_rows, step_rows), step_rows)
                outs[0][to, cols(0)] = (early[side, at, :] * factor).astype(jnp.bfloat16)
                return carry

            lax.fori_loop(0, EARLY // step_rows, scale_step, 0)
        rest_copy(0, first_peer(0, 1)).wait_recv()
    for j in range(1, max(tall, wide)):
        for m in range(2):
            if j < sizes[m][0]:
                at = pl.ds(0 if m else apart, kept * width - (0 if m else apart))
                block = part(m, owner_first(m, j), at)
                first_copy(m, j, block, block).wait_recv()

    def relay(c, carry):
        for j in range(1, max(tall, wide)):
            for m in range(2):
                if j < sizes[m][0]:
                    for k in range(1, sizes[m][1]):
                        next_copy(m, j, k, part(m, owner_first(m, j), cols(c))).start()
        return carry

    lax.fori_loop(0, kept, relay, 0)
    if gone:
        for m in range(2):
            first_copy(m, 1, near[m], near[m], 1).wait_recv()

        @pl.when(turn == 1)
        def _():
            pl.semaphore_wait(go, 1)

        for half in range(2):
            for m in range(2):
                held_copy(m, half).start()
        for m in range(2):
            held_copy(m, 0).wait_send()

        @pl.when(turn == 0)
        def _():
            pl.semaphore_signal(go, inc=1, device_id=sibling, device_id_type=MESH)

        for m in range(2):
            first_copy(m, 1, late[m], late[m], 2).wait_recv()

    for m in range(2):
        for c in range(max(0, chunks - SLOTS), chunks):
            all_peaks(m, c).wait_send()
        for k in range(1, sizes[m][0]):
            own = part(m, me, span(m, 0))
            first_copy(m, k, own, own).wait_send()
        for j in range(sizes[m][0]):
            at = span(m, j)
            for k in range(1, sizes[m][1]):
                next_copy(m, j, k, part(m, owner_first(m, j), at)).wait_send()
                next_copy(m, j, k, part(m, owner_next(m, j, k), at)).wait_recv()
    if gone:
        rest_copy(1, next_peer(0, 1)).wait_recv()
        for m in range(2):
            rest_copy(m, me).wait_send()
            held_copy(m, 1).wait_send()
            for half in range(2):
                held_copy(m, half).wait_recv()


def settle(rows, held_cols, late_cols, pieces, arrays, sides=()):
    ins = tuple(arrays) + tuple(sides)
    count = len(ins)

    def body(*refs):
        sem = refs[-1]
        near, far, late = refs[4:6], refs[6:8], refs[8:10]
        copies = []

        def add(src, dst):
            copies.append(pltpu.make_async_copy(src, dst, sem.at[len(copies)]))

        for a in range(len(arrays)):
            src, dst = refs[a], refs[count + a]
            if arrays[a].ndim == 1:
                add(src, dst)
                continue
            share = arrays[a].shape[0] // rows
            tall = share // pieces
            if not late_cols:
                for p in range(rows * pieces):
                    at = pl.ds(p * tall, tall)
                    add(src.at[at], dst.at[at])
                continue
            own = arrays[a].shape[1] - late_cols - held_cols
            me, first, second, last = around(rows, a)
            for owner, whole in ((me, True), (second, True), (first, False), (last, False)):
                for p in range(pieces):
                    at = pl.ds(pl.multiple_of(owner * share + p * tall, 16), tall)
                    if whole:
                        add(src.at[at], dst.at[at])
                    else:
                        add(src.at[at, pl.ds(0, own)], dst.at[at, pl.ds(0, own)])
            first_at = pl.ds(pl.multiple_of(first * share, 16), share)
            last_at = pl.ds(pl.multiple_of(last * share, 16), share)
            add(near[a], dst.at[first_at, pl.ds(own, held_cols)])
            add(late[a], dst.at[first_at, pl.ds(own + held_cols, late_cols)])
            add(far[a], dst.at[last_at, pl.ds(own, held_cols)])
        for copy in copies:
            copy.start()
        for copy in copies:
            copy.wait()

    size = sum(a.size * a.dtype.itemsize for a in arrays)
    return pl.pallas_call(
        body,
        out_shape=tuple(jax.ShapeDtypeStruct(a.shape, a.dtype) for a in arrays),
        in_specs=[pl.BlockSpec(memory_space=pl.ANY)] * count,
        out_specs=(pl.BlockSpec(memory_space=pltpu.HBM),) * len(arrays),
        scratch_shapes=[pltpu.SemaphoreType.DMA((2 * rows * pieces + 8,))],
        compiler_params=pltpu.CompilerParams(vmem_limit_bytes=SMALL),
        cost_estimate=pl.CostEstimate(flops=4 * size, bytes_accessed=2 * size, transcendentals=0),
    )(*ins)


def around(rows, m):
    me, y, x, turn = place(rows)
    turn = 1 - turn if m else turn
    by_x, by_y = y * 2 + (1 - x), (1 - y) * 2 + x
    near = (1 - turn) * by_x + turn * by_y
    side = (1 - turn) * by_y + turn * by_x
    return me, near, side, (1 - y) * 2 + (1 - x)


def complete(rows, served, late):
    share, late_cols = late[0].shape
    own = served[0].shape[1] - late_cols

    def body(*refs):
        sem = refs[-1]
        copies = []
        for m in range(2):
            at = pl.ds(pl.multiple_of(around(rows, m)[3] * share, 16), share)
            dst = refs[4 + m].at[at, pl.ds(own, late_cols)]
            copies.append(pltpu.make_async_copy(refs[2 + m], dst, sem.at[m]))
        for copy in copies:
            copy.start()
        for copy in copies:
            copy.wait()

    return pl.pallas_call(
        body,
        out_shape=tuple(jax.ShapeDtypeStruct(a.shape, a.dtype) for a in served),
        in_specs=[pl.BlockSpec(memory_space=pltpu.HBM)] * 2
        + [pl.BlockSpec(memory_space=pl.ANY)] * 2,
        out_specs=(pl.BlockSpec(memory_space=pltpu.HBM),) * 2,
        scratch_shapes=[pltpu.SemaphoreType.DMA((2,))],
        input_output_aliases={0: 0, 1: 1},
        compiler_params=pltpu.CompilerParams(vmem_limit_bytes=SMALL),
    )(*served, *late)


def solution(mesh):
    rows, lanes = mesh.shape["rows"], mesh.shape["tp"]

    def per_device(*args):
        arrays, norm_gain = args[:6], args[6]
        share, total = arrays[0].shape
        width = block_of(total, (LANES,))
        step_rows = block_of(share, (32, 16))
        chunks = total // width
        most = max(grid_of(rows))
        split = grid_of(rows) == (2, 2) and lanes % 2 == 0
        split = split and chunks > HELD + LATE and share > EARLY and EARLY % step_rows == 0
        pieces = 7 if share % (7 * step_rows) == 0 else 1
        held, gone = (HELD, LATE) if split else (0, 0)
        served = pltpu.VMEM((rows * share, total), jnp.bfloat16)
        column = pltpu.VMEM((total,), jnp.float32)
        sides = ()
        dma = pltpu.SemaphoreType.DMA
        more = []
        if split:
            held_side = pltpu.VMEM((share, held * width), jnp.bfloat16)
            sides = (held_side,) * 4 + (pltpu.VMEM((share, gone * width), jnp.bfloat16),) * 2
            more = [dma((2, 2)), dma((2, 2)), pltpu.SemaphoreType.REGULAR]
            more += [pltpu.VMEM((2, EARLY, width), jnp.float32)] + [dma((2,))] * 4
        got = pl.pallas_call(
            functools.partial(kernel, rows, width, step_rows, held, gone),
            out_shape=(served, served, column, column) + sides,
            in_specs=[pl.BlockSpec(memory_space=pltpu.HBM)] * 6
            + [pl.BlockSpec(memory_space=pltpu.VMEM)],
            out_specs=(pl.BlockSpec(memory_space=pltpu.VMEM),) * (4 + len(sides)),
            scratch_shapes=[
                pltpu.VMEM((2, 6, share, width), jnp.float32),
                pltpu.VMEM((2, 2, share, width), jnp.float32),
                pltpu.VMEM((2, SLOTS, rows, 1, width), jnp.float32),
                pltpu.VMEM((share, LANES), jnp.float32),
                dma((2, 2)),
                dma((pieces,)),
                dma((2, SLOTS)),
                dma((2, SLOTS)),
                dma((2, most - 1)),
                dma((3 if split else 1, 2, most - 1)),
                dma((most, 2, most - 1)),
                dma((most, 2, most - 1)),
            ]
            + more,
            compiler_params=pltpu.CompilerParams(
                collective_id=0, has_side_effects=True, vmem_limit_bytes=VMEM_LIMIT
            ),
        )(*arrays, norm_gain)
        if not split:
            return settle(rows, 0, 0, 2, got)

        def hop(m, late):
            hops = [
                (r * lanes + t, (r ^ (1 if (t + m) % 2 else 2)) * lanes + t)
                for r in range(rows)
                for t in range(lanes)
            ]
            return lax.ppermute(late, ("rows", "tp"), hops)

        late = [hop(m, got[8 + m]) for m in range(2)]
        done = settle(rows, held * width, gone * width, 2, got[:4], got[4:])
        return tuple(complete(rows, done[:2], late)) + tuple(done[2:])

    split = P("rows", "tp")
    return jax.shard_map(
        per_device,
        mesh=mesh,
        in_specs=(split,) * 6 + (P("rows"),),
        out_specs=(P(None, "tp"), P(None, "tp"), P("tp"), P("tp")),
        check_vma=False,
    )


HELD = 3
EARLY = 256
LATE = 3
SLOTS = 4
VMEM_LIMIT = 30 * 1024 * 1024
SMALL = 1024 * 1024
```

```python
import functools
import math

import jax
import jax.numpy as jnp
from jax import lax
from jax.experimental import pallas as pl
from jax.experimental.pallas import tpu as pltpu
from jax.sharding import PartitionSpec as P

learn_rate = 0.015
decay_rate = 0.1
tiny_value = 1e-08
MESH = pl.DeviceIdType.MESH
LANES = 128


def grid_of(rows):
    across = max(d for d in range(1, math.isqrt(rows) + 1) if rows % d == 0)
    return rows // across, across


def block_of(total, options):
    return next(b for b in options if total % b == 0)


def place(rows):
    tall, wide = grid_of(rows)
    me = lax.axis_index("rows")
    turn = lax.rem(lax.axis_index("tp"), 2) if tall == wide else 0
    return me, me // wide, lax.rem(me, wide), turn


def kernel(rows, width, step_rows, held, gone, *refs):
    ins, gains, outs, columns = refs[:6], refs[6], refs[7:9], refs[9:11]
    sides, rest = (refs[11:17], refs[17:]) if gone else ((), refs[11:])
    near, far, late = sides[:2], sides[2:4], sides[4:]
    stage, whole, peaks, gain = rest[:4]
    in_sem, piece_sem, peak_send, peak_recv = rest[4:8]
    first_send, first_recv, next_send, next_recv = rest[8:12]
    if gone:
        held_send, held_recv, go, early, early_send, early_recv, rest_send, rest_recv = rest[12:]
    tall, wide = grid_of(rows)
    share, total = ins[0].shape
    chunks = total // width
    kept = chunks - held - gone
    me, my_y, my_x, turn = place(rows)
    tp = lax.axis_index("tp")
    lead = (turn, 1 - turn)
    sizes = ((wide, tall), (tall, wide))

    def along_x(k):
        return my_y * wide + lax.rem(my_x + k, wide)

    def along_y(k):
        return lax.rem(my_y + k, tall) * wide + my_x

    def first_peer(m, k):
        return (1 - lead[m]) * along_x(k) + lead[m] * along_y(k)

    def next_peer(m, k):
        return (1 - lead[m]) * along_y(k) + lead[m] * along_x(k)

    def owner_next(m, j, k):
        down = (1 - lead[m]) * k + lead[m] * j
        left = (1 - lead[m]) * j + lead[m] * k
        return lax.rem(my_y + tall - down, tall) * wide + lax.rem(my_x + wide - left, wide)

    def owner_first(m, j):
        return first_peer(m, sizes[m][0] - j) if j else me

    def cols(c):
        return pl.ds(pl.multiple_of(c * width, LANES), width)

    def part(m, owner, at):
        return outs[m].at[pl.ds(pl.multiple_of(owner * share, step_rows), share), at]

    def load(m, c):
        slot = lax.rem(c, 2)
        return [
            pltpu.make_async_copy(
                ins[3 * m + a].at[:, cols(c)], stage.at[slot, 3 * m + a], in_sem.at[slot, m]
            )
            for a in range(3)
        ]

    def wait_load(m, c):
        slot = lax.rem(c, 2)
        block = stage.at[slot, pl.ds(3 * m, 3)]
        pltpu.make_async_copy(block, block, in_sem.at[slot, m]).wait()

    def send(src, dst, peer, send_sem, recv_sem):
        return pltpu.make_async_remote_copy(
            src_ref=src, dst_ref=dst, send_sem=send_sem, recv_sem=recv_sem,
            device_id={"rows": peer}, device_id_type=MESH,
        )

    def peak_copy(m, c, k):
        slot = lax.rem(c, SLOTS)
        ref = peaks.at[m, slot, me]
        return send(ref, ref, lax.rem(me + k, rows), peak_send.at[m, slot], peak_recv.at[m, slot])

    def all_peaks(m, c):
        slot = lax.rem(c, SLOTS)
        ref = peaks.at[m, slot, pl.ds(0, rows - 1)]
        return send(ref, ref, lax.rem(me + 1, rows), peak_send.at[m, slot], peak_recv.at[m, slot])

    def first_copy(m, k, src, dst, group=0):
        sems = first_send.at[m, k - 1], first_recv.at[group, m, k - 1]
        return send(src, dst, first_peer(m, k), *sems)

    def next_copy(m, j, k, ref):
        return send(ref, ref, next_peer(m, k), next_send.at[j, m, k - 1], next_recv.at[j, m, k - 1])

    def held_copy(m, half):
        at = pl.ds(0, share) if half is None else pl.ds(half * (share // 2), share // 2)
        sems = held_send.at[m, half or 0], held_recv.at[m, half or 0]
        return send(near[m].at[at], far[m].at[at], next_peer(m, 1), *sems)

    def early_copy(side):
        src, dst = whole.at[0, 0, pl.ds(0, EARLY)], early.at[side]
        peer = (first_peer, next_peer)[side](0, 1)
        return send(src, dst, peer, early_send.at[side], early_recv.at[side])

    def rest_copy(side, owner):
        at = pl.ds(pl.multiple_of(owner * share + EARLY, step_rows), share - EARLY)
        ref = outs[0].at[at, cols(0)]
        peer = (first_peer, next_peer)[side](0, 1)
        return send(ref, ref, peer, rest_send.at[side], rest_recv.at[side])

    pieces = piece_sem.shape[0]
    tall_piece = share // pieces
    for p in range(pieces):
        at = pl.ds(p * tall_piece, tall_piece)
        for a in range(3):
            pltpu.make_async_copy(
                ins[a].at[at, cols(0)], stage.at[0, a, at], piece_sem.at[p]
            ).start()

    barrier = pltpu.get_barrier_semaphore()
    for k in range(1, rows):
        pl.semaphore_signal(
            barrier, inc=1, device_id={"rows": lax.rem(me + k, rows)}, device_id_type=MESH
        )

    if gone:
        sibling = {"tp": tp + 1 - 2 * turn}
        pl.semaphore_signal(barrier, inc=1, device_id=sibling, device_id_type=MESH)

    zero = (jnp.zeros((8, LANES), jnp.float32),) * (width // LANES)

    def stepped(m, slot, low, high, most):
        def step(i, most):
            at = pl.ds(pl.multiple_of(i * step_rows, step_rows), step_rows)
            g = gain[at, :]
            found = []
            for t in range(width // LANES):
                lane = pl.ds(t * LANES, LANES)
                train, drift, spread = (stage[slot, 3 * m + a, at, lane] for a in range(3))
                new = train - learn_rate * (
                    drift / (jnp.sqrt(spread) + tiny_value) + decay_rate * train
                )
                new = new * g
                whole[slot, m, at, lane] = new
                tops = jnp.max(jnp.abs(new).reshape(step_rows // 8, 8, LANES), axis=0)
                found.append(jnp.maximum(most[t], tops))
            return tuple(found)

        return lax.fori_loop(low // step_rows, high // step_rows, step, most)

    def share_peaks(m, c, most):
        for t in range(width // LANES):
            peaks[m, c % SLOTS, me, :, pl.ds(t * LANES, LANES)] = jnp.max(most[t], axis=0, keepdims=True)

    def send_peaks(m, c):
        for k in range(1, rows):
            peak_copy(m, c, k).start()

    for start in range(0, share, LANES):
        count = min(LANES, share - start)
        line = gains[pl.ds(start, count)].reshape(1, count)
        gain[pl.ds(start, count), :] = jnp.broadcast_to(line, (LANES, count)).T

    most = zero
    for p in range(pieces):
        block = stage.at[0, pl.ds(0, 3), pl.ds(p * tall_piece, tall_piece)]
        pltpu.make_async_copy(block, block, piece_sem.at[p]).wait()
        if p == pieces // 2:
            for copy in load(1, 0):
                copy.start()
        most = stepped(0, 0, p * tall_piece, (p + 1) * tall_piece, most)
    share_peaks(0, 0, most)
    pl.semaphore_wait(barrier, rows if gone else rows - 1)
    send_peaks(0, 0)
    if gone:
        for side in range(2):
            early_copy(side).start()
    if chunks > 1:
        for copy in load(0, 1):
            copy.start()

    def update(m, c):
        slot = lax.rem(c, 2)
        wait_load(m, c)

        @pl.when(c + 1 < chunks)
        def _():
            for copy in load(m, c + 1):
                copy.start()

        most = stepped(m, slot, 0, share, zero)

        @pl.when(c >= SLOTS)
        def _():
            all_peaks(m, c - SLOTS).wait_send()

        share_peaks(m, c, most)
        send_peaks(m, c)

    update(1, 0)

    def finish(m, c, split=False):
        slot = lax.rem(c, 2)
        all_peaks(m, c).wait_recv()
        turn_slot = lax.rem(c, SLOTS)
        scale = peaks[m, turn_slot, 0]
        for r in range(1, rows):
            scale = jnp.maximum(scale, peaks[m, turn_slot, r])
        columns[m][cols(c)] = scale[0]
        factor = 1.0 / scale

        def step(i, carry):
            at = pl.ds(pl.multiple_of(i * step_rows, step_rows), step_rows)
            to = pl.ds(pl.multiple_of(me * share + i * step_rows, step_rows), step_rows)
            outs[m][to, cols(c)] = (whole[slot, m, at, :] * factor).astype(jnp.bfloat16)
            return carry

        lax.fori_loop(0, share // step_rows, step, 0)
        if split:
            for side in range(2):
                rest_copy(side, me).start()
            return
        own = part(m, me, cols(c))
        for k in range(1, sizes[m][0]):

            @pl.when(c < kept)
            def _(k=k):
                first_copy(m, k, own, own).start()

            if gone:

                @pl.when((c >= kept) & (c < kept + held))
                def _(k=k):
                    first_copy(m, k, own, near[m].at[:, cols(c - kept)], 1).start()

                @pl.when(c >= kept + held)
                def _(k=k):
                    first_copy(m, k, own, late[m].at[:, cols(c - kept - held)], 2).start()

        for k in range(1, sizes[m][1]):
            next_copy(m, 0, k, own).start()

    def body(c, carry):
        for m in range(2):
            update(m, c)
            finish(m, c - 1)
        return carry

    if gone:
        update(0, 1)
        finish(0, 0, True)
        update(1, 1)
        finish(1, 0)
        for side in range(2):
            early_copy(side).wait_send()
    lax.fori_loop(2 if gone else 1, chunks, body, 0)
    for m in range(2):
        finish(m, chunks - 1)

    apart = width if gone else 0

    def span(m, j):
        low = apart if j == 0 and m == 0 else 0
        high = total if j == 0 else kept * width
        return pl.ds(low, high - low)

    if gone:
        factor = 1.0 / columns[0][cols(0)].reshape(1, width)
        for side in range(2):
            owner = (first_peer, next_peer)[side](0, 1)
            early_copy(side).wait_recv()

            def scale_step(i, carry, side=side, owner=owner):
                at = pl.ds(pl.multiple_of(i * step_rows, step_rows), step_rows)
                to = pl.ds(pl.multiple_of(owner * share + i * step_rows, step_rows), step_rows)
                outs[0][to, cols(0)] = (early[side, at, :] * factor).astype(jnp.bfloat16)
                return carry

            lax.fori_loop(0, EARLY // step_rows, scale_step, 0)
        rest_copy(0, first_peer(0, 1)).wait_recv()
    for j in range(1, max(tall, wide)):
        for m in range(2):
            if j < sizes[m][0]:
                at = pl.ds(0 if m else apart, kept * width - (0 if m else apart))
                block = part(m, owner_first(m, j), at)
                first_copy(m, j, block, block).wait_recv()

    def relay(c, carry):
        for j in range(1, max(tall, wide)):
            for m in range(2):
                if j < sizes[m][0]:
                    for k in range(1, sizes[m][1]):
                        next_copy(m, j, k, part(m, owner_first(m, j), cols(c))).start()
        return carry

    lax.fori_loop(0, kept, relay, 0)
    if gone:
        for m in range(2):
            first_copy(m, 1, near[m], near[m], 1).wait_recv()

        @pl.when(turn == 1)
        def _():
            pl.semaphore_wait(go, 1)
            for m in range(2):
                held_copy(m, None).start()

        @pl.when(turn == 0)
        def _():
            for half in range(2):
                for m in range(2):
                    held_copy(m, half).start()
            for m in range(2):
                held_copy(m, 0).wait_send()
            pl.semaphore_signal(go, inc=1, device_id=sibling, device_id_type=MESH)

        for m in range(2):
            first_copy(m, 1, late[m], late[m], 2).wait_recv()

    for m in range(2):
        for c in range(max(0, chunks - SLOTS), chunks):
            all_peaks(m, c).wait_send()
        for k in range(1, sizes[m][0]):
            own = part(m, me, span(m, 0))
            first_copy(m, k, own, own).wait_send()
        for j in range(sizes[m][0]):
            at = span(m, j)
            for k in range(1, sizes[m][1]):
                next_copy(m, j, k, part(m, owner_first(m, j), at)).wait_send()
                next_copy(m, j, k, part(m, owner_next(m, j, k), at)).wait_recv()
    if gone:
        rest_copy(1, next_peer(0, 1)).wait_recv()
        for m in range(2):
            rest_copy(m, me).wait_send()

        @pl.when(turn == 0)
        def _():
            for m in range(2):
                held_copy(m, 1).wait_send()
                for half in range(2):
                    held_copy(m, half).wait_recv()

        @pl.when(turn == 1)
        def _():
            for m in range(2):
                held_copy(m, None).wait()


def settle(rows, held_cols, late_cols, pieces, arrays, sides=()):
    ins = tuple(arrays) + tuple(sides)
    count = len(ins)

    def body(*refs):
        sem = refs[-1]
        near, far, late = refs[4:6], refs[6:8], refs[8:10]
        copies = []

        def add(src, dst):
            copies.append(pltpu.make_async_copy(src, dst, sem.at[len(copies)]))

        for a in range(len(arrays)):
            src, dst = refs[a], refs[count + a]
            if arrays[a].ndim == 1:
                add(src, dst)
                continue
            share = arrays[a].shape[0] // rows
            tall = share // pieces
            if not late_cols:
                for p in range(rows * pieces):
                    at = pl.ds(p * tall, tall)
                    add(src.at[at], dst.at[at])
                continue
            own = arrays[a].shape[1] - late_cols - held_cols
            me, first, second, last = around(rows, a)
            for owner, whole in ((me, True), (second, True), (first, False), (last, False)):
                for p in range(pieces):
                    at = pl.ds(pl.multiple_of(owner * share + p * tall, 16), tall)
                    if whole:
                        add(src.at[at], dst.at[at])
                    else:
                        add(src.at[at, pl.ds(0, own)], dst.at[at, pl.ds(0, own)])
            first_at = pl.ds(pl.multiple_of(first * share, 16), share)
            last_at = pl.ds(pl.multiple_of(last * share, 16), share)
            add(near[a], dst.at[first_at, pl.ds(own, held_cols)])
            add(late[a], dst.at[first_at, pl.ds(own + held_cols, late_cols)])
            add(far[a], dst.at[last_at, pl.ds(own, held_cols)])
        for copy in copies:
            copy.start()
        for copy in copies:
            copy.wait()

    size = sum(a.size * a.dtype.itemsize for a in arrays)
    return pl.pallas_call(
        body,
        out_shape=tuple(jax.ShapeDtypeStruct(a.shape, a.dtype) for a in arrays),
        in_specs=[pl.BlockSpec(memory_space=pl.ANY)] * count,
        out_specs=(pl.BlockSpec(memory_space=pltpu.HBM),) * len(arrays),
        scratch_shapes=[pltpu.SemaphoreType.DMA((2 * rows * pieces + 8,))],
        compiler_params=pltpu.CompilerParams(vmem_limit_bytes=SMALL),
        cost_estimate=pl.CostEstimate(flops=4 * size, bytes_accessed=2 * size, transcendentals=0),
    )(*ins)


def around(rows, m):
    me, y, x, turn = place(rows)
    turn = 1 - turn if m else turn
    by_x, by_y = y * 2 + (1 - x), (1 - y) * 2 + x
    near = (1 - turn) * by_x + turn * by_y
    side = (1 - turn) * by_y + turn * by_x
    return me, near, side, (1 - y) * 2 + (1 - x)


def complete(rows, served, late):
    share, late_cols = late[0].shape
    own = served[0].shape[1] - late_cols

    def body(*refs):
        sem = refs[-1]
        copies = []
        for m in range(2):
            at = pl.ds(pl.multiple_of(around(rows, m)[3] * share, 16), share)
            dst = refs[4 + m].at[at, pl.ds(own, late_cols)]
            copies.append(pltpu.make_async_copy(refs[2 + m], dst, sem.at[m]))
        for copy in copies:
            copy.start()
        for copy in copies:
            copy.wait()

    return pl.pallas_call(
        body,
        out_shape=tuple(jax.ShapeDtypeStruct(a.shape, a.dtype) for a in served),
        in_specs=[pl.BlockSpec(memory_space=pltpu.HBM)] * 2
        + [pl.BlockSpec(memory_space=pl.ANY)] * 2,
        out_specs=(pl.BlockSpec(memory_space=pltpu.HBM),) * 2,
        scratch_shapes=[pltpu.SemaphoreType.DMA((2,))],
        input_output_aliases={0: 0, 1: 1},
        compiler_params=pltpu.CompilerParams(vmem_limit_bytes=SMALL),
    )(*served, *late)


def solution(mesh):
    rows, lanes = mesh.shape["rows"], mesh.shape["tp"]

    def per_device(*args):
        arrays, norm_gain = args[:6], args[6]
        share, total = arrays[0].shape
        width = block_of(total, (LANES,))
        step_rows = block_of(share, (32, 16))
        chunks = total // width
        most = max(grid_of(rows))
        split = grid_of(rows) == (2, 2) and lanes % 2 == 0
        split = split and chunks > HELD + LATE and share > EARLY and EARLY % step_rows == 0
        pieces = 7 if share % (7 * step_rows) == 0 else 1
        held, gone = (HELD, LATE) if split else (0, 0)
        served = pltpu.VMEM((rows * share, total), jnp.bfloat16)
        column = pltpu.VMEM((total,), jnp.float32)
        sides = ()
        dma = pltpu.SemaphoreType.DMA
        more = []
        if split:
            held_side = pltpu.VMEM((share, held * width), jnp.bfloat16)
            sides = (held_side,) * 4 + (pltpu.VMEM((share, gone * width), jnp.bfloat16),) * 2
            more = [dma((2, 2)), dma((2, 2)), pltpu.SemaphoreType.REGULAR]
            more += [pltpu.VMEM((2, EARLY, width), jnp.float32)] + [dma((2,))] * 4
        got = pl.pallas_call(
            functools.partial(kernel, rows, width, step_rows, held, gone),
            out_shape=(served, served, column, column) + sides,
            in_specs=[pl.BlockSpec(memory_space=pltpu.HBM)] * 6
            + [pl.BlockSpec(memory_space=pltpu.VMEM)],
            out_specs=(pl.BlockSpec(memory_space=pltpu.VMEM),) * (4 + len(sides)),
            scratch_shapes=[
                pltpu.VMEM((2, 6, share, width), jnp.float32),
                pltpu.VMEM((2, 2, share, width), jnp.float32),
                pltpu.VMEM((2, SLOTS, rows, 1, width), jnp.float32),
                pltpu.VMEM((share, LANES), jnp.float32),
                dma((2, 2)),
                dma((pieces,)),
                dma((2, SLOTS)),
                dma((2, SLOTS)),
                dma((2, most - 1)),
                dma((3 if split else 1, 2, most - 1)),
                dma((most, 2, most - 1)),
                dma((most, 2, most - 1)),
            ]
            + more,
            compiler_params=pltpu.CompilerParams(
                collective_id=0, has_side_effects=True, vmem_limit_bytes=VMEM_LIMIT
            ),
        )(*arrays, norm_gain)
        if not split:
            return settle(rows, 0, 0, 2, got)

        def hop(m, late):
            hops = [
                (r * lanes + t, (r ^ (1 if (t + m) % 2 else 2)) * lanes + t)
                for r in range(rows)
                for t in range(lanes)
            ]
            return lax.ppermute(late, ("rows", "tp"), hops)

        late = [hop(m, got[8 + m]) for m in range(2)]
        done = settle(rows, held * width, gone * width, 2, got[:4], got[4:])
        return tuple(complete(rows, done[:2], late)) + tuple(done[2:])

    split = P("rows", "tp")
    return jax.shard_map(
        per_device,
        mesh=mesh,
        in_specs=(split,) * 6 + (P("rows"),),
        out_specs=(P(None, "tp"), P(None, "tp"), P("tp"), P("tp")),
        check_vma=False,
    )


HELD = 4
EARLY = 256
LATE = 3
SLOTS = 4
VMEM_LIMIT = 31 * 1024 * 1024
SMALL = 1024 * 1024
```

```python
import functools
import math

import jax
import jax.numpy as jnp
from jax import lax
from jax.experimental import pallas as pl
from jax.experimental.pallas import tpu as pltpu
from jax.sharding import PartitionSpec as P

learn_rate = 0.015
decay_rate = 0.1
tiny_value = 1e-08
MESH = pl.DeviceIdType.MESH
LANES = 128


def grid_of(rows):
    across = max(d for d in range(1, math.isqrt(rows) + 1) if rows % d == 0)
    return rows // across, across


def block_of(total, options):
    return next(b for b in options if total % b == 0)


def place(rows):
    tall, wide = grid_of(rows)
    me = lax.axis_index("rows")
    turn = lax.rem(lax.axis_index("tp"), 2) if tall == wide else 0
    return me, me // wide, lax.rem(me, wide), turn


def kernel(rows, width, step_rows, held, gone, *refs):
    ins, gains, outs, columns = refs[:6], refs[6], refs[7:9], refs[9:11]
    sides, rest = (refs[11:17], refs[17:]) if gone else ((), refs[11:])
    near, far, late = sides[:2], sides[2:4], sides[4:]
    stage, whole, peaks, gain = rest[:4]
    in_sem, piece_sem, peak_send, peak_recv = rest[4:8]
    first_send, first_recv, next_send, next_recv = rest[8:12]
    if gone:
        held_send, held_recv, go, early, early_send, early_recv, rest_send, rest_recv = rest[12:]
    tall, wide = grid_of(rows)
    share, total = ins[0].shape
    chunks = total // width
    kept = chunks - held - gone
    me, my_y, my_x, turn = place(rows)
    tp = lax.axis_index("tp")
    lead = (turn, 1 - turn)
    sizes = ((wide, tall), (tall, wide))

    def along_x(k):
        return my_y * wide + lax.rem(my_x + k, wide)

    def along_y(k):
        return lax.rem(my_y + k, tall) * wide + my_x

    def first_peer(m, k):
        return (1 - lead[m]) * along_x(k) + lead[m] * along_y(k)

    def next_peer(m, k):
        return (1 - lead[m]) * along_y(k) + lead[m] * along_x(k)

    def owner_next(m, j, k):
        down = (1 - lead[m]) * k + lead[m] * j
        left = (1 - lead[m]) * j + lead[m] * k
        return lax.rem(my_y + tall - down, tall) * wide + lax.rem(my_x + wide - left, wide)

    def owner_first(m, j):
        return first_peer(m, sizes[m][0] - j) if j else me

    def cols(c):
        return pl.ds(pl.multiple_of(c * width, LANES), width)

    def part(m, owner, at):
        return outs[m].at[pl.ds(pl.multiple_of(owner * share, step_rows), share), at]

    def load(m, c):
        slot = lax.rem(c, 2)
        return [
            pltpu.make_async_copy(
                ins[3 * m + a].at[:, cols(c)], stage.at[slot, 3 * m + a], in_sem.at[slot, m]
            )
            for a in range(3)
        ]

    def wait_load(m, c):
        slot = lax.rem(c, 2)
        block = stage.at[slot, pl.ds(3 * m, 3)]
        pltpu.make_async_copy(block, block, in_sem.at[slot, m]).wait()

    def send(src, dst, peer, send_sem, recv_sem):
        return pltpu.make_async_remote_copy(
            src_ref=src, dst_ref=dst, send_sem=send_sem, recv_sem=recv_sem,
            device_id={"rows": peer}, device_id_type=MESH,
        )

    def peak_copy(m, c, k):
        slot = lax.rem(c, SLOTS)
        ref = peaks.at[m, slot, me]
        return send(ref, ref, lax.rem(me + k, rows), peak_send.at[m, slot], peak_recv.at[m, slot])

    def all_peaks(m, c):
        slot = lax.rem(c, SLOTS)
        ref = peaks.at[m, slot, pl.ds(0, rows - 1)]
        return send(ref, ref, lax.rem(me + 1, rows), peak_send.at[m, slot], peak_recv.at[m, slot])

    def first_copy(m, k, src, dst, group=0):
        sems = first_send.at[m, k - 1], first_recv.at[group, m, k - 1]
        return send(src, dst, first_peer(m, k), *sems)

    def next_copy(m, j, k, ref):
        return send(ref, ref, next_peer(m, k), next_send.at[j, m, k - 1], next_recv.at[j, m, k - 1])

    def held_copy(m, half):
        at = pl.ds(0, share) if half is None else pl.ds(half * (share // 2), share // 2)
        sems = held_send.at[m, half or 0], held_recv.at[m, half or 0]
        return send(near[m].at[at], far[m].at[at], next_peer(m, 1), *sems)

    def early_copy(side):
        src, dst = whole.at[0, 0, pl.ds(0, EARLY)], early.at[side]
        peer = (first_peer, next_peer)[side](0, 1)
        return send(src, dst, peer, early_send.at[side], early_recv.at[side])

    def rest_copy(side, owner):
        at = pl.ds(pl.multiple_of(owner * share + EARLY, step_rows), share - EARLY)
        ref = outs[0].at[at, cols(0)]
        peer = (first_peer, next_peer)[side](0, 1)
        return send(ref, ref, peer, rest_send.at[side], rest_recv.at[side])

    barrier = pltpu.get_barrier_semaphore()
    for k in range(1, rows):
        pl.semaphore_signal(
            barrier, inc=1, device_id={"rows": lax.rem(me + k, rows)}, device_id_type=MESH
        )

    if gone:
        sibling = {"tp": tp + 1 - 2 * turn}
        pl.semaphore_signal(barrier, inc=1, device_id=sibling, device_id_type=MESH)

    pieces = piece_sem.shape[0]
    tall_piece = share // pieces
    for p in range(pieces):
        at = pl.ds(p * tall_piece, tall_piece)
        for a in range(3):
            pltpu.make_async_copy(
                ins[a].at[at, cols(0)], stage.at[0, a, at], piece_sem.at[p]
            ).start()

    zero = (jnp.zeros((8, LANES), jnp.float32),) * (width // LANES)

    def stepped(m, slot, low, high, most):
        def step(i, most):
            at = pl.ds(pl.multiple_of(i * step_rows, step_rows), step_rows)
            g = gain[at, :]
            found = []
            for t in range(width // LANES):
                lane = pl.ds(t * LANES, LANES)
                train, drift, spread = (stage[slot, 3 * m + a, at, lane] for a in range(3))
                new = train - learn_rate * (
                    drift / (jnp.sqrt(spread) + tiny_value) + decay_rate * train
                )
                new = new * g
                whole[slot, m, at, lane] = new
                tops = jnp.max(jnp.abs(new).reshape(step_rows // 8, 8, LANES), axis=0)
                found.append(jnp.maximum(most[t], tops))
            return tuple(found)

        return lax.fori_loop(low // step_rows, high // step_rows, step, most)

    def share_peaks(m, c, most):
        for t in range(width // LANES):
            peaks[m, c % SLOTS, me, :, pl.ds(t * LANES, LANES)] = jnp.max(most[t], axis=0, keepdims=True)

    def send_peaks(m, c):
        for k in range(1, rows):
            peak_copy(m, c, k).start()

    for start in range(0, share, LANES):
        count = min(LANES, share - start)
        line = gains[pl.ds(start, count)].reshape(1, count)
        gain[pl.ds(start, count), :] = jnp.broadcast_to(line, (LANES, count)).T

    most = zero
    for p in range(pieces):
        block = stage.at[0, pl.ds(0, 3), pl.ds(p * tall_piece, tall_piece)]
        pltpu.make_async_copy(block, block, piece_sem.at[p]).wait()
        if p == pieces // 2:
            for copy in load(1, 0):
                copy.start()
        most = stepped(0, 0, p * tall_piece, (p + 1) * tall_piece, most)
    share_peaks(0, 0, most)
    pl.semaphore_wait(barrier, rows if gone else rows - 1)
    send_peaks(0, 0)
    if gone:
        for side in range(2):
            early_copy(side).start()
    if chunks > 1:
        for copy in load(0, 1):
            copy.start()

    def update(m, c):
        slot = lax.rem(c, 2)
        wait_load(m, c)

        @pl.when(c + 1 < chunks)
        def _():
            for copy in load(m, c + 1):
                copy.start()

        most = stepped(m, slot, 0, share, zero)

        @pl.when(c >= SLOTS)
        def _():
            all_peaks(m, c - SLOTS).wait_send()

        share_peaks(m, c, most)
        send_peaks(m, c)

    update(1, 0)

    def finish(m, c, split=False):
        slot = lax.rem(c, 2)
        all_peaks(m, c).wait_recv()
        turn_slot = lax.rem(c, SLOTS)
        scale = peaks[m, turn_slot, 0]
        for r in range(1, rows):
            scale = jnp.maximum(scale, peaks[m, turn_slot, r])
        columns[m][cols(c)] = scale[0]
        factor = 1.0 / scale

        def step(i, carry):
            at = pl.ds(pl.multiple_of(i * step_rows, step_rows), step_rows)
            to = pl.ds(pl.multiple_of(me * share + i * step_rows, step_rows), step_rows)
            outs[m][to, cols(c)] = (whole[slot, m, at, :] * factor).astype(jnp.bfloat16)
            return carry

        lax.fori_loop(0, share // step_rows, step, 0)
        if split:
            for side in range(2):
                rest_copy(side, me).start()
            return
        own = part(m, me, cols(c))
        for k in range(1, sizes[m][0]):

            @pl.when(c < kept)
            def _(k=k):
                first_copy(m, k, own, own).start()

            if gone:

                @pl.when((c >= kept) & (c < kept + held))
                def _(k=k):
                    first_copy(m, k, own, near[m].at[:, cols(c - kept)], 1).start()

                @pl.when(c >= kept + held)
                def _(k=k):
                    first_copy(m, k, own, late[m].at[:, cols(c - kept - held)], 2).start()

        for k in range(1, sizes[m][1]):
            next_copy(m, 0, k, own).start()

    def body(c, carry):
        for m in range(2):
            update(m, c)
            finish(m, c - 1)
        return carry

    if gone:
        update(0, 1)
        finish(0, 0, True)
        update(1, 1)
        finish(1, 0)
        for side in range(2):
            early_copy(side).wait_send()
    lax.fori_loop(2 if gone else 1, chunks, body, 0)
    for m in range(2):
        finish(m, chunks - 1)

    apart = width if gone else 0

    def span(m, j):
        low = apart if j == 0 and m == 0 else 0
        high = total if j == 0 else kept * width
        return pl.ds(low, high - low)

    if gone:
        factor = 1.0 / columns[0][cols(0)].reshape(1, width)
        for side in range(2):
            owner = (first_peer, next_peer)[side](0, 1)
            early_copy(side).wait_recv()

            def scale_step(i, carry, side=side, owner=owner):
                at = pl.ds(pl.multiple_of(i * step_rows, step_rows), step_rows)
                to = pl.ds(pl.multiple_of(owner * share + i * step_rows, step_rows), step_rows)
                outs[0][to, cols(0)] = (early[side, at, :] * factor).astype(jnp.bfloat16)
                return carry

            lax.fori_loop(0, EARLY // step_rows, scale_step, 0)
        rest_copy(0, first_peer(0, 1)).wait_recv()
    for j in range(1, max(tall, wide)):
        for m in range(2):
            if j < sizes[m][0]:
                at = pl.ds(0 if m else apart, kept * width - (0 if m else apart))
                block = part(m, owner_first(m, j), at)
                first_copy(m, j, block, block).wait_recv()

    def relay(c, carry):
        for j in range(1, max(tall, wide)):
            for m in range(2):
                if j < sizes[m][0]:
                    for k in range(1, sizes[m][1]):
                        next_copy(m, j, k, part(m, owner_first(m, j), cols(c))).start()
        return carry

    lax.fori_loop(0, kept, relay, 0)
    if gone:
        for m in range(2):
            first_copy(m, 1, near[m], near[m], 1).wait_recv()

        @pl.when(turn == 1)
        def _():
            pl.semaphore_wait(go, 1)
            for m in range(2):
                held_copy(m, None).start()

        @pl.when(turn == 0)
        def _():
            for half in range(2):
                for m in range(2):
                    held_copy(m, half).start()
            for m in range(2):
                held_copy(m, 0).wait_send()
            pl.semaphore_signal(go, inc=1, device_id=sibling, device_id_type=MESH)

        for m in range(2):
            first_copy(m, 1, late[m], late[m], 2).wait_recv()

    for m in range(2):
        for c in range(max(0, chunks - SLOTS), chunks):
            all_peaks(m, c).wait_send()
        for k in range(1, sizes[m][0]):
            own = part(m, me, span(m, 0))
            first_copy(m, k, own, own).wait_send()
        for j in range(sizes[m][0]):
            at = span(m, j)
            for k in range(1, sizes[m][1]):
                next_copy(m, j, k, part(m, owner_first(m, j), at)).wait_send()
                next_copy(m, j, k, part(m, owner_next(m, j, k), at)).wait_recv()
    if gone:
        rest_copy(1, next_peer(0, 1)).wait_recv()
        for m in range(2):
            rest_copy(m, me).wait_send()

        @pl.when(turn == 0)
        def _():
            for m in range(2):
                held_copy(m, 1).wait_send()
                for half in range(2):
                    held_copy(m, half).wait_recv()

        @pl.when(turn == 1)
        def _():
            for m in range(2):
                held_copy(m, None).wait()


def settle(rows, held_cols, late_cols, pieces, arrays, sides=()):
    ins = tuple(arrays) + tuple(sides)
    count = len(ins)

    def body(*refs):
        sem = refs[-1]
        near, far, late = refs[4:6], refs[6:8], refs[8:10]
        copies = []

        def add(src, dst):
            copies.append(pltpu.make_async_copy(src, dst, sem.at[len(copies)]))

        for a in range(len(arrays)):
            src, dst = refs[a], refs[count + a]
            if arrays[a].ndim == 1:
                add(src, dst)
                continue
            share = arrays[a].shape[0] // rows
            tall = share // pieces
            if not late_cols:
                for p in range(rows * pieces):
                    at = pl.ds(p * tall, tall)
                    add(src.at[at], dst.at[at])
                continue
            own = arrays[a].shape[1] - late_cols - held_cols
            me, first, second, last = around(rows, a)
            for owner, whole in ((me, True), (second, True), (first, False), (last, False)):
                for p in range(pieces):
                    at = pl.ds(pl.multiple_of(owner * share + p * tall, 16), tall)
                    if whole:
                        add(src.at[at], dst.at[at])
                    else:
                        add(src.at[at, pl.ds(0, own)], dst.at[at, pl.ds(0, own)])
            first_at = pl.ds(pl.multiple_of(first * share, 16), share)
            last_at = pl.ds(pl.multiple_of(last * share, 16), share)
            add(near[a], dst.at[first_at, pl.ds(own, held_cols)])
            add(late[a], dst.at[first_at, pl.ds(own + held_cols, late_cols)])
            add(far[a], dst.at[last_at, pl.ds(own, held_cols)])
        for copy in copies:
            copy.start()
        for copy in copies:
            copy.wait()

    size = sum(a.size * a.dtype.itemsize for a in arrays)
    return pl.pallas_call(
        body,
        out_shape=tuple(jax.ShapeDtypeStruct(a.shape, a.dtype) for a in arrays),
        in_specs=[pl.BlockSpec(memory_space=pl.ANY)] * count,
        out_specs=(pl.BlockSpec(memory_space=pltpu.HBM),) * len(arrays),
        scratch_shapes=[pltpu.SemaphoreType.DMA((2 * rows * pieces + 8,))],
        compiler_params=pltpu.CompilerParams(vmem_limit_bytes=SMALL),
        cost_estimate=pl.CostEstimate(flops=4 * size, bytes_accessed=2 * size, transcendentals=0),
    )(*ins)


def around(rows, m):
    me, y, x, turn = place(rows)
    turn = 1 - turn if m else turn
    by_x, by_y = y * 2 + (1 - x), (1 - y) * 2 + x
    near = (1 - turn) * by_x + turn * by_y
    side = (1 - turn) * by_y + turn * by_x
    return me, near, side, (1 - y) * 2 + (1 - x)


def complete(rows, served, late):
    share, late_cols = late[0].shape
    own = served[0].shape[1] - late_cols

    def body(*refs):
        sem = refs[-1]
        copies = []
        for m in range(2):
            at = pl.ds(pl.multiple_of(around(rows, m)[3] * share, 16), share)
            dst = refs[4 + m].at[at, pl.ds(own, late_cols)]
            copies.append(pltpu.make_async_copy(refs[2 + m], dst, sem.at[m]))
        for copy in copies:
            copy.start()
        for copy in copies:
            copy.wait()

    return pl.pallas_call(
        body,
        out_shape=tuple(jax.ShapeDtypeStruct(a.shape, a.dtype) for a in served),
        in_specs=[pl.BlockSpec(memory_space=pltpu.HBM)] * 2
        + [pl.BlockSpec(memory_space=pl.ANY)] * 2,
        out_specs=(pl.BlockSpec(memory_space=pltpu.HBM),) * 2,
        scratch_shapes=[pltpu.SemaphoreType.DMA((2,))],
        input_output_aliases={0: 0, 1: 1},
        compiler_params=pltpu.CompilerParams(vmem_limit_bytes=SMALL),
    )(*served, *late)


def solution(mesh):
    rows, lanes = mesh.shape["rows"], mesh.shape["tp"]

    def per_device(*args):
        arrays, norm_gain = args[:6], args[6]
        share, total = arrays[0].shape
        width = block_of(total, (LANES,))
        step_rows = block_of(share, (32, 16))
        chunks = total // width
        most = max(grid_of(rows))
        split = grid_of(rows) == (2, 2) and lanes % 2 == 0
        split = split and chunks > HELD + LATE + 1 and share > EARLY and EARLY % step_rows == 0
        pieces = 7 if share % (7 * step_rows) == 0 else 1
        held, gone = (HELD, LATE) if split else (0, 0)
        served = pltpu.VMEM((rows * share, total), jnp.bfloat16)
        column = pltpu.VMEM((total,), jnp.float32)
        sides = ()
        dma = pltpu.SemaphoreType.DMA
        more = []
        if split:
            held_side = pltpu.VMEM((share, held * width), jnp.bfloat16)
            sides = (held_side,) * 4 + (pltpu.VMEM((share, gone * width), jnp.bfloat16),) * 2
            more = [dma((2, 2)), dma((2, 2)), pltpu.SemaphoreType.REGULAR]
            more += [pltpu.VMEM((2, EARLY, width), jnp.float32)] + [dma((2,))] * 4
        got = pl.pallas_call(
            functools.partial(kernel, rows, width, step_rows, held, gone),
            out_shape=(served, served, column, column) + sides,
            in_specs=[pl.BlockSpec(memory_space=pltpu.HBM)] * 6
            + [pl.BlockSpec(memory_space=pltpu.VMEM)],
            out_specs=(pl.BlockSpec(memory_space=pltpu.VMEM),) * (4 + len(sides)),
            scratch_shapes=[
                pltpu.VMEM((2, 6, share, width), jnp.float32),
                pltpu.VMEM((2, 2, share, width), jnp.float32),
                pltpu.VMEM((2, SLOTS, rows, 1, width), jnp.float32),
                pltpu.VMEM((share, LANES), jnp.float32),
                dma((2, 2)),
                dma((pieces,)),
                dma((2, SLOTS)),
                dma((2, SLOTS)),
                dma((2, most - 1)),
                dma((3 if split else 1, 2, most - 1)),
                dma((most, 2, most - 1)),
                dma((most, 2, most - 1)),
            ]
            + more,
            compiler_params=pltpu.CompilerParams(
                collective_id=0, has_side_effects=True, vmem_limit_bytes=VMEM_LIMIT
            ),
        )(*arrays, norm_gain)
        if not split:
            return settle(rows, 0, 0, 2, got)

        def hop(m, late):
            hops = [
                (r * lanes + t, (r ^ (1 if (t + m) % 2 else 2)) * lanes + t)
                for r in range(rows)
                for t in range(lanes)
            ]
            return lax.ppermute(late, ("rows", "tp"), hops)

        late = [hop(m, got[8 + m]) for m in range(2)]
        done = settle(rows, held * width, gone * width, 2, got[:4], got[4:])
        return tuple(complete(rows, done[:2], late)) + tuple(done[2:])

    split = P("rows", "tp")
    return jax.shard_map(
        per_device,
        mesh=mesh,
        in_specs=(split,) * 6 + (P("rows"),),
        out_specs=(P(None, "tp"), P(None, "tp"), P("tp"), P("tp")),
        check_vma=False,
    )


HELD = 4
EARLY = 256
LATE = 3
SLOTS = 4
VMEM_LIMIT = 31 * 1024 * 1024
SMALL = 1024 * 1024
```

```python
import functools
import math

import jax
import jax.numpy as jnp
from jax import lax
from jax.experimental import pallas as pl
from jax.experimental.pallas import tpu as pltpu
from jax.sharding import PartitionSpec as P

learn_rate = 0.015
decay_rate = 0.1
tiny_value = 1e-08
MESH = pl.DeviceIdType.MESH
LANES = 128


def grid_of(rows):
    across = max(d for d in range(1, math.isqrt(rows) + 1) if rows % d == 0)
    return rows // across, across


def block_of(total, options):
    return next(b for b in options if total % b == 0)


def place(rows):
    tall, wide = grid_of(rows)
    me = lax.axis_index("rows")
    turn = lax.rem(lax.axis_index("tp"), 2) if tall == wide else 0
    return me, me // wide, lax.rem(me, wide), turn


def kernel(rows, width, step_rows, held, gone, *refs):
    ins, gains, outs, columns = refs[:6], refs[6], refs[7:9], refs[9:11]
    sides, rest = (refs[11:17], refs[17:]) if gone else ((), refs[11:])
    near, far, late = sides[:2], sides[2:4], sides[4:]
    stage, whole, peaks, gain = rest[:4]
    in_sem, piece_sem, peak_send, peak_recv = rest[4:8]
    first_send, first_recv, next_send, next_recv = rest[8:12]
    if gone:
        held_send, held_recv, go, early, early_send, early_recv, rest_send, rest_recv = rest[12:]
    tall, wide = grid_of(rows)
    share, total = ins[0].shape
    chunks = total // width
    kept = chunks - held - gone
    me, my_y, my_x, turn = place(rows)
    tp = lax.axis_index("tp")
    lead = (turn, 1 - turn)
    sizes = ((wide, tall), (tall, wide))

    def along_x(k):
        return my_y * wide + lax.rem(my_x + k, wide)

    def along_y(k):
        return lax.rem(my_y + k, tall) * wide + my_x

    def first_peer(m, k):
        return (1 - lead[m]) * along_x(k) + lead[m] * along_y(k)

    def next_peer(m, k):
        return (1 - lead[m]) * along_y(k) + lead[m] * along_x(k)

    def owner_next(m, j, k):
        down = (1 - lead[m]) * k + lead[m] * j
        left = (1 - lead[m]) * j + lead[m] * k
        return lax.rem(my_y + tall - down, tall) * wide + lax.rem(my_x + wide - left, wide)

    def owner_first(m, j):
        return first_peer(m, sizes[m][0] - j) if j else me

    def cols(c):
        return pl.ds(pl.multiple_of(c * width, LANES), width)

    def part(m, owner, at):
        return outs[m].at[pl.ds(pl.multiple_of(owner * share, step_rows), share), at]

    def load(m, c):
        slot = lax.rem(c, 2)
        return [
            pltpu.make_async_copy(
                ins[3 * m + a].at[:, cols(c)], stage.at[slot, 3 * m + a], in_sem.at[slot, m]
            )
            for a in range(3)
        ]

    def wait_load(m, c):
        slot = lax.rem(c, 2)
        block = stage.at[slot, pl.ds(3 * m, 3)]
        pltpu.make_async_copy(block, block, in_sem.at[slot, m]).wait()

    def send(src, dst, peer, send_sem, recv_sem):
        return pltpu.make_async_remote_copy(
            src_ref=src, dst_ref=dst, send_sem=send_sem, recv_sem=recv_sem,
            device_id={"rows": peer}, device_id_type=MESH,
        )

    def peak_copy(m, c, k):
        slot = lax.rem(c, SLOTS)
        ref = peaks.at[m, slot, me]
        return send(ref, ref, lax.rem(me + k, rows), peak_send.at[m, slot], peak_recv.at[m, slot])

    def all_peaks(m, c):
        slot = lax.rem(c, SLOTS)
        ref = peaks.at[m, slot, pl.ds(0, rows - 1)]
        return send(ref, ref, lax.rem(me + 1, rows), peak_send.at[m, slot], peak_recv.at[m, slot])

    def first_copy(m, k, src, dst, group=0):
        sems = first_send.at[m, k - 1], first_recv.at[group, m, k - 1]
        return send(src, dst, first_peer(m, k), *sems)

    def next_copy(m, j, k, ref):
        return send(ref, ref, next_peer(m, k), next_send.at[j, m, k - 1], next_recv.at[j, m, k - 1])

    def held_copy(m, half):
        at = pl.ds(0, share) if half is None else pl.ds(half * (share // 2), share // 2)
        sems = held_send.at[m, half or 0], held_recv.at[m, half or 0]
        return send(near[m].at[at], far[m].at[at], next_peer(m, 1), *sems)

    def early_copy(side):
        src, dst = whole.at[0, 0, pl.ds(0, EARLY)], early.at[side]
        peer = (first_peer, next_peer)[side](0, 1)
        return send(src, dst, peer, early_send.at[side], early_recv.at[side])

    def rest_copy(side, owner):
        at = pl.ds(pl.multiple_of(owner * share + EARLY, step_rows), share - EARLY)
        ref = outs[0].at[at, cols(0)]
        peer = (first_peer, next_peer)[side](0, 1)
        return send(ref, ref, peer, rest_send.at[side], rest_recv.at[side])

    barrier = pltpu.get_barrier_semaphore()
    for k in range(1, rows):
        pl.semaphore_signal(
            barrier, inc=1, device_id={"rows": lax.rem(me + k, rows)}, device_id_type=MESH
        )

    if gone:
        sibling = {"tp": tp + 1 - 2 * turn}
        pl.semaphore_signal(barrier, inc=1, device_id=sibling, device_id_type=MESH)

    pieces = piece_sem.shape[0]
    tall_piece = share // pieces
    for p in range(pieces):
        at = pl.ds(p * tall_piece, tall_piece)
        for a in range(3):
            pltpu.make_async_copy(
                ins[a].at[at, cols(0)], stage.at[0, a, at], piece_sem.at[p]
            ).start()

    zero = (jnp.zeros((8, LANES), jnp.float32),) * (width // LANES)

    def stepped(m, slot, low, high, most):
        def step(i, most):
            at = pl.ds(pl.multiple_of(i * step_rows, step_rows), step_rows)
            g = gain[at, :]
            found = []
            for t in range(width // LANES):
                lane = pl.ds(t * LANES, LANES)
                train, drift, spread = (stage[slot, 3 * m + a, at, lane] for a in range(3))
                new = train - learn_rate * (
                    drift / (spread * lax.rsqrt(spread) + tiny_value) + decay_rate * train
                )
                new = new * g
                whole[slot, m, at, lane] = new
                tops = jnp.max(jnp.abs(new).reshape(step_rows // 8, 8, LANES), axis=0)
                found.append(jnp.maximum(most[t], tops))
            return tuple(found)

        return lax.fori_loop(low // step_rows, high // step_rows, step, most)

    def share_peaks(m, c, most):
        for t in range(width // LANES):
            peaks[m, c % SLOTS, me, :, pl.ds(t * LANES, LANES)] = jnp.max(most[t], axis=0, keepdims=True)

    def send_peaks(m, c):
        for k in range(1, rows):
            peak_copy(m, c, k).start()

    for start in range(0, share, LANES):
        count = min(LANES, share - start)
        line = gains[pl.ds(start, count)].reshape(1, count)
        gain[pl.ds(start, count), :] = jnp.broadcast_to(line, (LANES, count)).T

    most = zero
    for p in range(pieces):
        block = stage.at[0, pl.ds(0, 3), pl.ds(p * tall_piece, tall_piece)]
        pltpu.make_async_copy(block, block, piece_sem.at[p]).wait()
        if p == pieces // 2:
            for copy in load(1, 0):
                copy.start()
        most = stepped(0, 0, p * tall_piece, (p + 1) * tall_piece, most)
    share_peaks(0, 0, most)
    pl.semaphore_wait(barrier, rows if gone else rows - 1)
    send_peaks(0, 0)
    if gone:
        for side in range(2):
            early_copy(side).start()
    if chunks > 1:
        for copy in load(0, 1):
            copy.start()

    def update(m, c):
        slot = lax.rem(c, 2)
        wait_load(m, c)

        @pl.when(c + 1 < chunks)
        def _():
            for copy in load(m, c + 1):
                copy.start()

        most = stepped(m, slot, 0, share, zero)

        @pl.when(c >= SLOTS)
        def _():
            all_peaks(m, c - SLOTS).wait_send()

        share_peaks(m, c, most)
        send_peaks(m, c)

    update(1, 0)

    def finish(m, c, split=False):
        slot = lax.rem(c, 2)
        all_peaks(m, c).wait_recv()
        turn_slot = lax.rem(c, SLOTS)
        scale = peaks[m, turn_slot, 0]
        for r in range(1, rows):
            scale = jnp.maximum(scale, peaks[m, turn_slot, r])
        columns[m][cols(c)] = scale[0]
        factor = 1.0 / scale

        def step(i, carry):
            at = pl.ds(pl.multiple_of(i * step_rows, step_rows), step_rows)
            to = pl.ds(pl.multiple_of(me * share + i * step_rows, step_rows), step_rows)
            outs[m][to, cols(c)] = (whole[slot, m, at, :] * factor).astype(jnp.bfloat16)
            return carry

        if split:
            lax.fori_loop(EARLY // step_rows, share // step_rows, step, 0)
            for side in range(2):
                rest_copy(side, me).start()
            lax.fori_loop(0, EARLY // step_rows, step, 0)
            return
        lax.fori_loop(0, share // step_rows, step, 0)
        own = part(m, me, cols(c))
        for k in range(1, sizes[m][0]):

            @pl.when(c < kept)
            def _(k=k):
                first_copy(m, k, own, own).start()

            if gone:

                @pl.when((c >= kept) & (c < kept + held))
                def _(k=k):
                    first_copy(m, k, own, near[m].at[:, cols(c - kept)], 1).start()

                @pl.when(c >= kept + held)
                def _(k=k):
                    first_copy(m, k, own, late[m].at[:, cols(c - kept - held)], 2).start()

        for k in range(1, sizes[m][1]):
            next_copy(m, 0, k, own).start()

    def body(c, carry):
        for m in range(2):
            update(m, c)
            finish(m, c - 1)
        return carry

    if gone:
        update(0, 1)
        finish(0, 0, True)
        update(1, 1)
        finish(1, 0)
        for side in range(2):
            early_copy(side).wait_send()
    lax.fori_loop(2 if gone else 1, chunks, body, 0)
    for m in range(2):
        finish(m, chunks - 1)

    apart = width if gone else 0

    def span(m, j):
        low = apart if j == 0 and m == 0 else 0
        high = total if j == 0 else kept * width
        return pl.ds(low, high - low)

    if gone:
        factor = 1.0 / columns[0][cols(0)].reshape(1, width)
        for side in range(2):
            owner = (first_peer, next_peer)[side](0, 1)
            early_copy(side).wait_recv()

            def scale_step(i, carry, side=side, owner=owner):
                at = pl.ds(pl.multiple_of(i * step_rows, step_rows), step_rows)
                to = pl.ds(pl.multiple_of(owner * share + i * step_rows, step_rows), step_rows)
                outs[0][to, cols(0)] = (early[side, at, :] * factor).astype(jnp.bfloat16)
                return carry

            lax.fori_loop(0, EARLY // step_rows, scale_step, 0)
        rest_copy(0, first_peer(0, 1)).wait_recv()
    for j in range(1, max(tall, wide)):
        for m in range(2):
            if j < sizes[m][0]:
                at = pl.ds(0 if m else apart, kept * width - (0 if m else apart))
                block = part(m, owner_first(m, j), at)
                first_copy(m, j, block, block).wait_recv()

    def relay(c, carry):
        for j in range(1, max(tall, wide)):
            for m in range(2):
                if j < sizes[m][0]:
                    for k in range(1, sizes[m][1]):
                        next_copy(m, j, k, part(m, owner_first(m, j), cols(c))).start()
        return carry

    lax.fori_loop(0, kept, relay, 0)
    if gone:
        for m in range(2):
            first_copy(m, 1, near[m], near[m], 1).wait_recv()

        @pl.when(turn == 1)
        def _():
            pl.semaphore_wait(go, 1)
            for m in range(2):
                held_copy(m, None).start()

        @pl.when(turn == 0)
        def _():
            for half in range(2):
                for m in range(2):
                    held_copy(m, half).start()
            for m in range(2):
                held_copy(m, 0).wait_send()
            pl.semaphore_signal(go, inc=1, device_id=sibling, device_id_type=MESH)

        for m in range(2):
            first_copy(m, 1, late[m], late[m], 2).wait_recv()

    for m in range(2):
        for c in range(max(0, chunks - SLOTS), chunks):
            all_peaks(m, c).wait_send()
        for k in range(1, sizes[m][0]):
            own = part(m, me, span(m, 0))
            first_copy(m, k, own, own).wait_send()
        for j in range(sizes[m][0]):
            at = span(m, j)
            for k in range(1, sizes[m][1]):
                next_copy(m, j, k, part(m, owner_first(m, j), at)).wait_send()
                next_copy(m, j, k, part(m, owner_next(m, j, k), at)).wait_recv()
    if gone:
        rest_copy(1, next_peer(0, 1)).wait_recv()
        for m in range(2):
            rest_copy(m, me).wait_send()

        @pl.when(turn == 0)
        def _():
            for m in range(2):
                held_copy(m, 1).wait_send()
                for half in range(2):
                    held_copy(m, half).wait_recv()

        @pl.when(turn == 1)
        def _():
            for m in range(2):
                held_copy(m, None).wait()


def settle(rows, held_cols, late_cols, pieces, arrays, sides=()):
    ins = tuple(arrays) + tuple(sides)
    count = len(ins)

    def body(*refs):
        sem = refs[-1]
        near, far, late = refs[4:6], refs[6:8], refs[8:10]
        copies = []

        def add(src, dst):
            copies.append(pltpu.make_async_copy(src, dst, sem.at[len(copies)]))

        for a in range(len(arrays)):
            src, dst = refs[a], refs[count + a]
            if arrays[a].ndim == 1:
                add(src, dst)
                continue
            share = arrays[a].shape[0] // rows
            tall = share // pieces
            if not late_cols:
                for p in range(rows * pieces):
                    at = pl.ds(p * tall, tall)
                    add(src.at[at], dst.at[at])
                continue
            own = arrays[a].shape[1] - late_cols - held_cols
            me, first, second, last = around(rows, a)
            for owner, whole in ((me, True), (second, True), (first, False), (last, False)):
                for p in range(pieces):
                    at = pl.ds(pl.multiple_of(owner * share + p * tall, 16), tall)
                    if whole:
                        add(src.at[at], dst.at[at])
                    else:
                        add(src.at[at, pl.ds(0, own)], dst.at[at, pl.ds(0, own)])
            first_at = pl.ds(pl.multiple_of(first * share, 16), share)
            last_at = pl.ds(pl.multiple_of(last * share, 16), share)
            add(near[a], dst.at[first_at, pl.ds(own, held_cols)])
            add(late[a], dst.at[first_at, pl.ds(own + held_cols, late_cols)])
            add(far[a], dst.at[last_at, pl.ds(own, held_cols)])
        for copy in copies:
            copy.start()
        for copy in copies:
            copy.wait()

    size = sum(a.size * a.dtype.itemsize for a in arrays)
    return pl.pallas_call(
        body,
        out_shape=tuple(jax.ShapeDtypeStruct(a.shape, a.dtype) for a in arrays),
        in_specs=[pl.BlockSpec(memory_space=pl.ANY)] * count,
        out_specs=(pl.BlockSpec(memory_space=pltpu.HBM),) * len(arrays),
        scratch_shapes=[pltpu.SemaphoreType.DMA((2 * rows * pieces + 8,))],
        compiler_params=pltpu.CompilerParams(vmem_limit_bytes=SMALL),
        cost_estimate=pl.CostEstimate(flops=4 * size, bytes_accessed=2 * size, transcendentals=0),
    )(*ins)


def around(rows, m):
    me, y, x, turn = place(rows)
    turn = 1 - turn if m else turn
    by_x, by_y = y * 2 + (1 - x), (1 - y) * 2 + x
    near = (1 - turn) * by_x + turn * by_y
    side = (1 - turn) * by_y + turn * by_x
    return me, near, side, (1 - y) * 2 + (1 - x)


def complete(rows, served, late):
    share, late_cols = late[0].shape
    own = served[0].shape[1] - late_cols

    def body(*refs):
        sem = refs[-1]
        copies = []
        for m in range(2):
            at = pl.ds(pl.multiple_of(around(rows, m)[3] * share, 16), share)
            dst = refs[4 + m].at[at, pl.ds(own, late_cols)]
            copies.append(pltpu.make_async_copy(refs[2 + m], dst, sem.at[m]))
        for copy in copies:
            copy.start()
        for copy in copies:
            copy.wait()

    return pl.pallas_call(
        body,
        out_shape=tuple(jax.ShapeDtypeStruct(a.shape, a.dtype) for a in served),
        in_specs=[pl.BlockSpec(memory_space=pltpu.HBM)] * 2
        + [pl.BlockSpec(memory_space=pl.ANY)] * 2,
        out_specs=(pl.BlockSpec(memory_space=pltpu.HBM),) * 2,
        scratch_shapes=[pltpu.SemaphoreType.DMA((2,))],
        input_output_aliases={0: 0, 1: 1},
        compiler_params=pltpu.CompilerParams(vmem_limit_bytes=SMALL),
    )(*served, *late)


def solution(mesh):
    rows, lanes = mesh.shape["rows"], mesh.shape["tp"]

    def per_device(*args):
        arrays, norm_gain = args[:6], args[6]
        share, total = arrays[0].shape
        width = block_of(total, (LANES,))
        step_rows = block_of(share, (32, 16))
        chunks = total // width
        most = max(grid_of(rows))
        split = grid_of(rows) == (2, 2) and lanes % 2 == 0
        split = split and chunks > HELD + LATE + 1 and share > EARLY and EARLY % step_rows == 0
        pieces = 7 if share % (7 * step_rows) == 0 else 1
        held, gone = (HELD, LATE) if split else (0, 0)
        served = pltpu.VMEM((rows * share, total), jnp.bfloat16)
        column = pltpu.VMEM((total,), jnp.float32)
        sides = ()
        dma = pltpu.SemaphoreType.DMA
        more = []
        if split:
            held_side = pltpu.VMEM((share, held * width), jnp.bfloat16)
            sides = (held_side,) * 4 + (pltpu.VMEM((share, gone * width), jnp.bfloat16),) * 2
            more = [dma((2, 2)), dma((2, 2)), pltpu.SemaphoreType.REGULAR]
            more += [pltpu.VMEM((2, EARLY, width), jnp.float32)] + [dma((2,))] * 4
        got = pl.pallas_call(
            functools.partial(kernel, rows, width, step_rows, held, gone),
            out_shape=(served, served, column, column) + sides,
            in_specs=[pl.BlockSpec(memory_space=pltpu.HBM)] * 6
            + [pl.BlockSpec(memory_space=pltpu.VMEM)],
            out_specs=(pl.BlockSpec(memory_space=pltpu.VMEM),) * (4 + len(sides)),
            scratch_shapes=[
                pltpu.VMEM((2, 6, share, width), jnp.float32),
                pltpu.VMEM((2, 2, share, width), jnp.float32),
                pltpu.VMEM((2, SLOTS, rows, 1, width), jnp.float32),
                pltpu.VMEM((share, LANES), jnp.float32),
                dma((2, 2)),
                dma((pieces,)),
                dma((2, SLOTS)),
                dma((2, SLOTS)),
                dma((2, most - 1)),
                dma((3 if split else 1, 2, most - 1)),
                dma((most, 2, most - 1)),
                dma((most, 2, most - 1)),
            ]
            + more,
            compiler_params=pltpu.CompilerParams(
                collective_id=0, has_side_effects=True, vmem_limit_bytes=VMEM_LIMIT
            ),
        )(*arrays, norm_gain)
        if not split:
            return settle(rows, 0, 0, 2, got)

        def hop(m, late):
            hops = [
                (r * lanes + t, (r ^ (1 if (t + m) % 2 else 2)) * lanes + t)
                for r in range(rows)
                for t in range(lanes)
            ]
            return lax.ppermute(late, ("rows", "tp"), hops)

        late = [hop(m, got[8 + m]) for m in range(2)]
        done = settle(rows, held * width, gone * width, 2, got[:4], got[4:])
        return tuple(complete(rows, done[:2], late)) + tuple(done[2:])

    split = P("rows", "tp")
    return jax.shard_map(
        per_device,
        mesh=mesh,
        in_specs=(split,) * 6 + (P("rows"),),
        out_specs=(P(None, "tp"), P(None, "tp"), P("tp"), P("tp")),
        check_vma=False,
    )


HELD = 4
EARLY = 256
LATE = 3
SLOTS = 4
VMEM_LIMIT = 31 * 1024 * 1024
SMALL = 1024 * 1024
```
